32 devices in a mesh: front: 8 (over y, x, core), sub: 4 (over z).
Axes of the slice: x: 2, y: 2, z: 4, core: 2. Of those that a mesh axis runs over, the one named last changes fastest.
Arguments:
- row_values: float32 [4096, 1024], P(('front', 'sub')), may hold values from -0.12 to 0.12
- front_of_row: int32 [4096, 1], P(('front', 'sub')), may hold values from 0 to 7; in each aligned block of 128 rows (0 to 127, 128 to 255, ...) at most 32 rows name the same one
- child_factors: float32 [16, 512, 512], P('front', 'sub'), as said below
- child_columns: int32 [16, 512], P('front'), may hold values from 0 to 1023, as said below
- damping: float32 [8, 1024], P('front'), may hold values from 0.5 to 2
Outputs:
- front_factor: float32 [8, 1024, 1024], P('front', 'sub')
The draws below stay inside these ranges and needn't reach their ends.
Inputs may be any that keep to these rules, and one draw needn't show every extreme that they name: `front_of_row`: among the 128 rows of one device, at most 32 name the same front, and some device's block reaches this bound. `child_factors`: each block is upper triangular with a positive diagonal. `child_columns`: each row names 512 distinct columns.
All inputs are finite; a program needn't handle non-finite values.
Results may differ from the reference program's by a relative error of at most 0.0003.
Values sent between devices are 32-bit elements; how exact they have to be, the bound alone decides.
No kernel may reach another device: no remote copies, remote signals or barrier semaphores. Data moves between devices by JAX's collectives and lax.ppermute only.
A program may use at most 64 MiB of HBM per device.

```python
import math
import jax
import jax.numpy as jnp
import numpy as np
from jax import lax

CONTRIB = 512
F = 1024
ROWS_SRC = 128
FRONTS = 8
MOST = 32
ROWS = 4096
N_FRONT = 8
N_SUB = 4


def draw_child_factors(key, part):
    key_diag = jax.random.fold_in(key, 11)
    key_off = jax.random.fold_in(key, 12)
    shape = (2 * FRONTS, CONTRIB, CONTRIB)
    diagonal = jnp.exp(jax.random.uniform(key_diag, (2 * FRONTS, CONTRIB), jnp.float32, jnp.log(0.5), jnp.log(2.0)))
    offdiag = jnp.clip(jax.random.normal(key_off, shape, jnp.float32), -5.0, 5.0) * (0.5 / jnp.sqrt(jnp.float32(CONTRIB)))
    upper_mask = jnp.triu(jnp.ones((CONTRIB, CONTRIB), jnp.float32), 1)
    eye_mask = jnp.eye(CONTRIB, dtype=jnp.float32)
    return (offdiag * upper_mask[None] + diagonal[:, :, None] * eye_mask[None]).astype(jnp.float32)


def draw_child_columns(key, part):
    key_score = jax.random.fold_in(key, 21)
    scores = jax.random.randint(key_score, (2 * FRONTS, F), 0, 2 ** 19, jnp.int32)
    distinct = scores * F + jnp.arange(F, dtype=jnp.int32)[None, :]
    permuted = jnp.argsort(distinct, axis=1, stable=True).astype(jnp.int32)
    return permuted[:, :CONTRIB]


def level_of(key, extent, cuts, low, largest):
    gain = 1.0
    for position, parts in cuts:
        steps = jax.random.uniform(jax.random.fold_in(jax.random.fold_in(key, 6), position), (parts,), jnp.float32, low / len(cuts), largest / len(cuts))
        gain = gain * jnp.repeat(jnp.exp(steps), extent[position] // parts).reshape((-1,) + (1,) * (len(extent) - 1 - position))
    return gain


def shared_out(stream_key, own, number, rows, number_of, top, reach, skew):
    order = jax.random.permutation(stream_key, number_of)
    crowded, usual = load_shares(number_of, rows * top, reach, skew, True), load_shares(number_of, rows * top, reach, skew, False)
    places = jnp.arange(number_of)

    def named(tallies, rotation):
        used = int((tallies > 0).sum())
        fixed = max(1, used // 4)
        passed = fixed + (places - fixed + rotation * (used - fixed)) % max(1, number_of - fixed)
        return jnp.zeros((number_of,), jnp.int32).at[order[jnp.where(places < fixed, places, passed)]].set(jnp.asarray(tallies, jnp.int32))

    tallies = jnp.where(number % 4 == 0, named(crowded, number // 4), named(usual, number - number // 4 - 1))
    mixed = jax.random.permutation(jax.random.fold_in(own, 3), number_of)
    giver, taker = mixed[0:number_of // 2 * 2:2], mixed[1:number_of // 2 * 2:2]
    slack = jnp.minimum(tallies[giver] - 1, reach - tallies[taker]) // 2
    slack = jnp.where((giver == order[0]) | (taker == order[0]) | (tallies[taker] == 0), 0, jnp.maximum(slack, 0))
    passed = jax.random.randint(jax.random.fold_in(own, 4), (number_of // 2,), 0, 1 << 20) % (slack + 1)
    tallies = tallies.at[giver].add(-passed).at[taker].add(passed)
    items = jnp.searchsorted(jnp.cumsum(tallies), jnp.arange(rows * top), side="right").astype(jnp.int32)
    listing = items.reshape(top, rows).T
    listing = listing[jax.random.permutation(jax.random.fold_in(own, 1), rows)]
    rotation = jax.random.randint(jax.random.fold_in(own, 2), (rows, 1), 0, top)
    return jnp.take_along_axis(listing, (jnp.arange(top)[None, :] + rotation) % top, axis=1)


def load_shares(number_of, total, limit, slope, full):
    portions = [(1 << 20) // math.isqrt(rank ** slope) + 1 for rank in range(1, number_of + 1)]
    largest = limit if full else min(limit, max(-(-total // number_of), total * portions[0] // sum(portions)))
    least = 1 if total - largest >= number_of - 1 else 0
    holding, spare = [largest] + [least] * (number_of - 1), total - largest - least * (number_of - 1)
    while spare > 0:
        free = [i for i in range(1, number_of) if holding[i] < largest] or [i for i in range(1, number_of) if holding[i] < limit]
        pool, remaining = sum([portions[i] for i in free]), spare
        for i in free:
            addition = min(limit - holding[i], max(1, remaining * portions[i] // pool), spare)
            holding[i] = holding[i] + addition
            spare = spare - addition
    return np.array(holding)


def noise(rng, extent, scale, limit, pieces=(), held_as=jnp.bfloat16):
    level = level_of(rng, extent, pieces, -0.22, 0.18) if pieces else 1.0
    values = jax.random.normal(rng, extent, jnp.float32) * scale * level
    return jnp.minimum(jnp.maximum(values, -limit), limit).astype(held_as)


def setup_inputs(seed: int = 0) -> dict:
    key_list = jax.random.split(jax.random.key(seed), 6)
    row_values = noise(key_list[0], (ROWS, F), 0.02, 0.12, ((0, 32),), jnp.float32)
    front_of_row_keys = jax.random.split(jax.random.fold_in(key_list[1], 1), ROWS // ROWS_SRC)
    front_of_row_turns = jax.random.permutation(jax.random.fold_in(key_list[1], 3), ROWS // ROWS_SRC)
    front_of_row = jax.vmap(lambda own, number: shared_out(jax.random.fold_in(key_list[1], 2), own, number, ROWS_SRC, FRONTS, 1, MOST, 2))(front_of_row_keys, front_of_row_turns).reshape((ROWS, 1))
    child_factors = draw_child_factors(jax.random.fold_in(key_list[5], 71), 0)
    child_columns = draw_child_columns(jax.random.fold_in(key_list[5], 71), 0)
    damping = jnp.clip(jnp.exp(math.log(2.0) - 1.3862944 * jax.random.uniform(key_list[4], (FRONTS, F), jnp.float32) ** level_of(key_list[4], (FRONTS, F), ((0, 8),), -0.2, 0.2)), 0.5, 2.0)
    return {"row_values": row_values, "front_of_row": front_of_row, "child_factors": child_factors, "child_columns": child_columns, "damping": damping}


HIGHEST = lax.Precision.HIGHEST

def gram_product(matrix):
    return lax.dot_general(matrix.astype(jnp.float32), matrix.astype(jnp.float32), (((0,), (0,)), ((), ())), precision=HIGHEST, preferred_element_type=jnp.float32)

def reference(row_values, front_of_row, child_factors, child_columns, damping):
    destination = front_of_row[:, 0].astype(jnp.int32)
    sorted_rows = jnp.argsort(destination, stable=True).astype(jnp.int32)
    counts = jnp.bincount(destination, length=FRONTS).astype(jnp.int32)
    starts = (jnp.cumsum(counts) - counts).astype(jnp.int32)
    capacity = MOST * N_FRONT * N_SUB
    padded_order = jnp.concatenate([sorted_rows, jnp.zeros((capacity,), jnp.int32)])
    columns = jnp.arange(F, dtype=jnp.int32)

    def factor_front(front_index):
        row_index = lax.dynamic_slice(padded_order, (starts[front_index],), (capacity,))
        is_live = jnp.arange(capacity, dtype=jnp.int32) < counts[front_index]
        front_rows = jnp.where(is_live[:, None], row_values[row_index], jnp.float32(0.0))
        gram_matrix = gram_product(front_rows)
        for child_index in range(2):
            child = child_factors[2 * front_index + child_index]
            mapping = child_columns[2 * front_index + child_index]
            spread = (mapping[:, None] == columns[None, :]).astype(jnp.float32)
            placed = jnp.dot(child.astype(jnp.float32), spread.astype(jnp.float32), precision=HIGHEST, preferred_element_type=jnp.float32)
            gram_matrix = gram_matrix + gram_product(placed)
        weight = damping[front_index]
        gram_matrix = gram_matrix + jnp.diag(weight * weight)
        return jnp.linalg.cholesky(gram_matrix).T
    return lax.map(factor_front, jnp.arange(FRONTS, dtype=jnp.int32))
```

```python
import functools

import jax
import jax.numpy as jnp
from jax import lax
from jax.experimental import pallas as pl
from jax.experimental.pallas import tpu as pltpu
from jax.sharding import PartitionSpec as P

HIGHEST = lax.Precision.HIGHEST
f32 = jnp.float32

def dot(a, b, ca=1, cb=0):
    return lax.dot_general(a, b, (((ca,), (cb,)), ((), ())), precision=HIGHEST, preferred_element_type=f32)

def rowb(v, j):
    return jnp.broadcast_to(v[j:j + 1, :], v.shape)

def laneb(v, c):
    return jnp.broadcast_to(v[:, c:c + 1], v.shape)

def factor_tile(load, store_r, store_w, n=128, width=16):
    lane = lax.broadcasted_iota(jnp.int32, (8, n), 1)
    sub = lax.broadcasted_iota(jnp.int32, (8, n), 0)
    lane1 = lax.broadcasted_iota(jnp.int32, (1, n), 1)
    tiles = n // 8
    per = width // 8
    x = [load(m) for m in range(tiles)]
    for blk in range(n // width):
        lo = blk * width
        first = blk * per
        own = [x[first + v] for v in range(per)]
        t = list(own)
        w = [jnp.where(lane < lo, own[v], jnp.where(lane == sub + (lo + 8 * v), 1.0, 0.0)) for v in range(per)]
        b = [[laneb(own[v], lo + c) for c in range(width)] for v in range(per)]
        later = [[laneb(x[m], lo + c) for c in range(width)] for m in range(first + per, tiles)]
        for j in range(width):
            pv, jj = divmod(j, 8)
            d = rowb(b[pv][j], jj)
            inv = 1.0 / d
            root = lax.rsqrt(d)
            trow, wrow = rowb(t[pv], jj), rowb(w[pv], jj)
            store_r(lo + j, jnp.where(lane1 >= lo + j, (trow * root)[0:1], 0.0))
            store_w(lo + j, (wrow * root)[0:1])
            tp, wp = trow * inv, wrow * inv
            bp = {c: rowb(b[pv][c], jj) * inv for c in range(j + 1, width)}
            for v in range(per):
                col = b[v][j]
                if v == pv:
                    here = sub == jj
                    col = jnp.where(here, -1.0, col)
                    t[v] = jnp.where(here, 0.0, t[v]) - col * tp
                    w[v] = jnp.where(here, 0.0, w[v]) - col * wp
                    for c in range(j + 1, width):
                        b[v][c] = jnp.where(here, 0.0, b[v][c]) - col * bp[c]
                else:
                    t[v] = t[v] - col * tp
                    w[v] = w[v] - col * wp
                    for c in range(j + 1, width):
                        b[v][c] = b[v][c] - col * bp[c]
        z = [jnp.where(lane < lo + width, w[v], t[v]) for v in range(per)]
        for i, m in enumerate(range(first + per, tiles)):
            terms = [later[i][c] * rowb(z[c // 8], c % 8) for c in range(width)]
            while len(terms) > 1:
                terms = [terms[q] + terms[q + 1] for q in range(0, len(terms) - 1, 2)] + ([terms[-1]] if len(terms) % 2 else [])
            x[m] = jnp.where((lane >= lo) & (lane < lo + width), 0.0, x[m]) - terms[0]

def block_kernel(nprev, width, *refs):
    g_ref = refs[0]
    prev = refs[1:1 + nprev]
    r_ref, d_ref, w_ref = refs[1 + nprev:]
    rows, cols = g_ref.shape
    half = 128
    u = g_ref[...]
    for t in range(nprev):
        off = rows * (nprev - t)
        u = u - dot(prev[t][:, off:off + rows], prev[t][:, off:], 0, 0)
    r_ref[...] = u
    for p in range(rows // half):
        a = p * half
        if p:
            r_ref[a:a + half, a:] = r_ref[a:a + half, a:] - dot(r_ref[0:a, a:a + half], r_ref[0:a, a:], 0, 0)
        d_ref[...] = r_ref[a:a + half, a:a + half]
        def store_r(i, v): r_ref[a + i:a + i + 1, a:a + half] = v
        def store_w(i, v): w_ref[i:i + 1, :] = v
        factor_tile(lambda m: d_ref[8 * m:8 * m + 8, :], store_r, store_w, half, width)
        if a:
            r_ref[a:a + half, 0:a] = jnp.zeros((half, a), f32)
        if a + half < cols:
            r_ref[a:a + half, a + half:] = dot(w_ref[...], r_ref[a:a + half, a + half:])

def chol_block(g, prev, width=16):
    n = len(prev)
    return pl.pallas_call(
        functools.partial(block_kernel, n, width),
        out_shape=jax.ShapeDtypeStruct(g.shape, f32),
        in_specs=[pl.BlockSpec(memory_space=pltpu.VMEM)] * (n + 1),
        out_specs=pl.BlockSpec(memory_space=pltpu.VMEM),
        scratch_shapes=[pltpu.VMEM((128, 128), f32), pltpu.VMEM((128, 128), f32)],
        compiler_params=pltpu.CompilerParams(vmem_limit_bytes=48 << 20),
        name="factor_block",
    )(g, *prev)

def chol_full(gs, width=16):
    rs = []
    for g in gs:
        rs.append(chol_block(g, rs, width))
    return rs


def cross_product(left_cols, right_cols):
    return lax.dot_general(
        left_cols,
        right_cols,
        (((0,), (0,)), ((), ())),
        precision=HIGHEST,
        preferred_element_type=jnp.float32,
    )


def local(row_values, front_of_row, child_factors, child_columns, damping):
    fronts = lax.axis_size("front")
    rows_held, front_width = row_values.shape
    capacity = 2 * rows_held // fronts
    destination = front_of_row[:, 0]
    onehot = (destination[:, None] == jnp.arange(fronts, dtype=jnp.int32)[None, :]).astype(
        jnp.int32
    )
    position = jnp.sum((jnp.cumsum(onehot, axis=0) - onehot) * onehot, axis=1)
    slot_of = destination * capacity + position
    source = (
        jnp.full((fronts * capacity,), rows_held, jnp.int32)
        .at[slot_of]
        .set(jnp.arange(rows_held, dtype=jnp.int32))
    )
    padded = jnp.concatenate([row_values, jnp.zeros((1, front_width), row_values.dtype)], axis=0)
    outgoing = padded[source]
    received = lax.all_to_all(outgoing, "front", split_axis=0, concat_axis=0, tiled=True)
    columns = jnp.arange(front_width, dtype=jnp.int32)
    spread = (child_columns[:, :, None] == columns[None, None, :]).astype(jnp.float32)
    placed = jnp.einsum(
        "jrc,jcf->jrf", child_factors, spread, precision=HIGHEST, preferred_element_type=jnp.float32
    )
    stacked = jnp.concatenate([placed.reshape(-1, front_width), received], axis=0)
    sub_count = lax.axis_size("sub")
    block_rows = front_width // sub_count
    own_index = lax.axis_index("sub")
    weight = damping[0]
    summed_gram = lax.psum(cross_product(stacked, stacked), "sub")
    summed_gram = summed_gram + jnp.diag(weight * weight)
    blocks = [
        summed_gram[start : start + block_rows, start:]
        for start in range(0, front_width, block_rows)
    ]
    factors = chol_full(blocks)
    full_factor = jnp.concatenate(
        [jnp.pad(r, ((0, 0), (front_width - r.shape[1], 0))) for r in factors], axis=0
    )
    own_rows = lax.dynamic_slice_in_dim(full_factor, own_index * block_rows, block_rows, 0)
    return own_rows[None]


def solution(mesh):
    in_specs = (
        P(("front", "sub"), None),
        P(("front", "sub"), None),
        P("front", "sub", None),
        P("front", None),
        P("front", None),
    )
    out_specs = P("front", "sub", None)
    return jax.shard_map(local, mesh=mesh, in_specs=in_specs, out_specs=out_specs, check_vma=False)
```

```python
import functools

import jax
import jax.numpy as jnp
from jax import lax
from jax.experimental import pallas as pl
from jax.experimental.pallas import tpu as pltpu
from jax.sharding import PartitionSpec as P

HIGHEST = lax.Precision.HIGHEST


def cost(us):
    return pl.CostEstimate(flops=int(us * 5e8), bytes_accessed=0, transcendentals=0)

f32 = jnp.float32

def dot(a, b, ca=1, cb=0):
    return lax.dot_general(a, b, (((ca,), (cb,)), ((), ())), precision=HIGHEST, preferred_element_type=f32)

def rowb(v, j):
    return jnp.broadcast_to(v[j:j + 1, :], v.shape)

def factor_tile(x, store_r, store_w, spread_ref, n=128, width=16):
    lane = lax.broadcasted_iota(jnp.int32, (8, n), 1)
    sub = lax.broadcasted_iota(jnp.int32, (8, n), 0)
    lane1 = lax.broadcasted_iota(jnp.int32, (1, n), 1)
    per = width // 8
    blocks = n // width
    def spread(v, c, slot):
        spread_ref[slot] = jnp.broadcast_to(v[:, c:c + 1], v.shape)
        return spread_ref[slot]
    own = [x[8 * v:8 * v + 8, :] for v in range(per)]
    nxt = [x[width + 8 * v:width + 8 * v + 8, :] for v in range(per)]
    rest = x[2 * width:, :]
    for blk in range(blocks):
        lo = blk * width
        base = (blk % 2) * 2 * per * width
        t = list(own)
        w = [jnp.where(lane < lo, own[v], jnp.where(lane == sub + (lo + 8 * v), 1.0, 0.0)) for v in range(per)]
        b = [[None] * width for _ in range(per)]
        for c in range(width):
            for v in range(per):
                b[v][c] = spread(own[v], lo + c, base + v * width + c)
        last = blk == blocks - 1
        if not last:
            later = [[None] * width for _ in range(per)]
            for c in range(width):
                for v in range(per):
                    later[v][c] = spread(nxt[v], lo + c, base + (per + v) * width + c)
        for j in range(width):
            pv, jj = divmod(j, 8)
            here = sub == jj
            d = rowb(b[pv][j], jj)
            inv = 1.0 / d
            root = lax.rsqrt(d)
            cols = [b[v][j] for v in range(per)]
            cols[pv] = jnp.where(here, -1.0, cols[pv])
            for c in range(j + 1, width):
                row = rowb(b[pv][c], jj)
                if c == j + 1:
                    for v in range(per):
                        kept = jnp.where(here, 0.0, b[v][c]) if v == pv else b[v][c]
                        b[v][c] = kept - (cols[v] * row) * inv
                else:
                    row = row * inv
                    for v in range(per):
                        kept = jnp.where(here, 0.0, b[v][c]) if v == pv else b[v][c]
                        b[v][c] = kept - cols[v] * row
            trow, wrow = rowb(t[pv], jj), rowb(w[pv], jj)
            store_r(lo + j, jnp.where(lane1 >= lo + j, (trow * root)[0:1], 0.0))
            store_w(lo + j, (wrow * root)[0:1])
            tp, wp = trow * inv, wrow * inv
            for v in range(per):
                if last and v < pv:
                    continue
                for a, p in ((t, tp), (w, wp)):
                    kept = jnp.where(here, 0.0, a[v]) if v == pv else a[v]
                    a[v] = kept - cols[v] * p
        if last:
            break
        inside = (lane >= lo) & (lane < lo + width)
        z = [jnp.where(lane < lo + width, w[v], t[v]) for v in range(per)]
        new = []
        for v in range(per):
            terms = [later[v][c] * rowb(z[c // 8], c % 8) for c in range(width)]
            while len(terms) > 1:
                terms = [terms[q] + terms[q + 1] for q in range(0, len(terms), 2)]
            new.append(jnp.where(inside, 0.0, nxt[v]) - terms[0])
        own = new
        if rest.shape[0]:
            parts = [jnp.zeros((lo, n), f32)] if lo else []
            parts += z + [jnp.zeros((n - lo - width, n), f32)]
            zpad = jnp.concatenate(parts, axis=0)
            lane_r = lax.broadcasted_iota(jnp.int32, rest.shape, 1)
            rest = jnp.where((lane_r >= lo) & (lane_r < lo + width), 0.0, rest) - dot(rest, zpad)
            nxt = [rest[8 * v:8 * v + 8, :] for v in range(per)]
            rest = rest[width:, :]


def block_kernel(nprev, width, *refs):
    g_ref = refs[0]
    prev = refs[1:1 + nprev]
    r_ref, w_ref, spread_ref = refs[1 + nprev:]
    rows, cols = g_ref.shape
    half = 128
    u = g_ref[...]
    for t in range(nprev):
        off = rows * (nprev - t)
        u = u - dot(prev[t][:, off:off + rows], prev[t][:, off:], 0, 0)
    r_ref[...] = u
    for p in range(rows // half):
        a = p * half
        if p:
            r_ref[a:a + half, a:] = r_ref[a:a + half, a:] - dot(r_ref[0:a, a:a + half], r_ref[0:a, a:], 0, 0)
        tile = r_ref[a:a + half, a:a + half]
        def store_r(i, v): r_ref[a + i:a + i + 1, a:a + half] = v
        def store_w(i, v): w_ref[i:i + 1, :] = v
        factor_tile(tile, store_r, store_w, spread_ref, half, width)
        if a:
            r_ref[a:a + half, 0:a] = jnp.zeros((half, a), f32)
        if a + half < cols:
            r_ref[a:a + half, a + half:] = dot(w_ref[...], r_ref[a:a + half, a + half:])

def chol_block(g, prev, width=16):
    n = len(prev)
    return pl.pallas_call(
        functools.partial(block_kernel, n, width),
        out_shape=jax.ShapeDtypeStruct(g.shape, f32),
        in_specs=[pl.BlockSpec(memory_space=pltpu.VMEM)] * (n + 1),
        out_specs=pl.BlockSpec(memory_space=pltpu.VMEM),
        scratch_shapes=[pltpu.VMEM((128, 128), f32), pltpu.VMEM((width * width // 2, 8, 128), f32)],
        compiler_params=pltpu.CompilerParams(vmem_limit_bytes=48 << 20),
        cost_estimate=cost(6),
        name="factor_block",
    )(g, *prev)

def split3(x):
    high = x.astype(jnp.bfloat16)
    rest = x - high.astype(f32)
    mid = rest.astype(jnp.bfloat16)
    low = (rest - mid.astype(f32)).astype(jnp.bfloat16)
    return high, mid, low


def pick_exact(onehot, x, ca, cb, onehot_left):
    total = None
    for piece in split3(x):
        a, b = (onehot, piece) if onehot_left else (piece, onehot)
        part = lax.dot_general(a, b, (((ca,), (cb,)), ((), ())), preferred_element_type=f32)
        total = part if total is None else total + part
    return total


def route_kernel(capacity, rows_ref, col_ref, out_ref):
    n = rows_ref.shape[0]
    slots = out_ref.shape[0]
    down = lax.broadcasted_iota(jnp.int32, (n, n), 0)
    across = lax.broadcasted_iota(jnp.int32, (n, n), 1)
    column = jnp.broadcast_to(col_ref[...], (n, n))
    row = jnp.sum(jnp.where(down == across, column, 0), axis=0, keepdims=True)
    earlier = (column == row) & (down < across)
    position = jnp.sum(earlier.astype(jnp.int32), axis=0, keepdims=True)
    slot = row * capacity + position
    pick = lax.broadcasted_iota(jnp.int32, (slots, n), 0) == slot
    out_ref[...] = pick_exact(pick.astype(f32).astype(jnp.bfloat16), rows_ref[...], 1, 0, True)


def route(row_values, front_of_row, fronts):
    n, width = row_values.shape
    capacity = 2 * n // fronts
    return pl.pallas_call(
        functools.partial(route_kernel, capacity),
        out_shape=jax.ShapeDtypeStruct((fronts * capacity, width), f32),
        in_specs=[pl.BlockSpec(memory_space=pltpu.VMEM)] * 2,
        out_specs=pl.BlockSpec(memory_space=pltpu.VMEM),
        cost_estimate=cost(3),
        name="route",
    )(row_values, front_of_row)


def children_kernel(block, nparts, *refs):
    parts = refs[:nparts]
    columns_ref, damping_ref, own_ref = refs[nparts:nparts + 3]
    outs = refs[nparts + 3:-1]
    placed_ref = refs[-1]
    width = placed_ref.shape[1]
    kids, rows, contrib = parts[0].shape
    for c in range(kids):
        spread = lax.broadcasted_iota(jnp.int32, (width, contrib), 0) == columns_ref[c:c + 1, :]
        spread = spread.astype(f32).astype(jnp.bfloat16)
        for q in range(nparts):
            at = (c * nparts + q) * rows
            placed_ref[at:at + rows, :] = pick_exact(spread, parts[q][c], 1, 1, False)
    weight = damping_ref[...]
    for s, out_ref in enumerate(outs):
        lo = s * block
        down = lax.broadcasted_iota(jnp.int32, out_ref.shape, 0)
        across = lax.broadcasted_iota(jnp.int32, out_ref.shape, 1)
        diag = jnp.where(down == across, weight[:, lo:] * weight[:, lo:], 0.0)
        kids_part = dot(placed_ref[:, lo:lo + block], placed_ref[:, lo:], 0, 0)
        out_ref[...] = diag + kids_part + dot(own_ref[:, lo:lo + block], own_ref[:, lo:], 0, 0)


def block_shapes(width, block):
    return [jax.ShapeDtypeStruct((block, width - lo), f32) for lo in range(0, width, block)]


def children_gram(parts, columns, damping, own, block):
    width = damping.shape[1]
    kids, rows, _ = parts[0].shape
    shapes = block_shapes(width, block)
    return pl.pallas_call(
        functools.partial(children_kernel, block, len(parts)),
        out_shape=shapes,
        in_specs=[pl.BlockSpec(memory_space=pltpu.VMEM)] * (len(parts) + 3),
        out_specs=[pl.BlockSpec(memory_space=pltpu.VMEM)] * len(shapes),
        scratch_shapes=[pltpu.VMEM((kids * rows * len(parts), width), f32)],
        compiler_params=pltpu.CompilerParams(vmem_limit_bytes=48 << 20),
        cost_estimate=cost(19),
        name="children_gram",
    )(*parts, columns, damping, own)


def dot16(a, b, ca, cb):
    return lax.dot_general(a, b, (((ca,), (cb,)), ((), ())), preferred_element_type=f32)


def rays_kernel(block, nblocks, nparts, *refs):
    grams = refs[:nblocks]
    parts = refs[nblocks:nblocks + nparts]
    outs = refs[nblocks + nparts:-2]
    high_ref, low_ref = refs[-2:]
    rows = parts[0].shape[0]
    for q, part in enumerate(parts):
        x = part[...]
        high = x.astype(jnp.bfloat16)
        high_ref[q * rows:(q + 1) * rows, :] = high
        low_ref[q * rows:(q + 1) * rows, :] = (x - high.astype(f32)).astype(jnp.bfloat16)
    for s in range(nblocks):
        lo = s * block
        left_high, left_low = high_ref[:, lo:lo + block], low_ref[:, lo:lo + block]
        small = dot16(left_high, low_ref[:, lo:], 0, 0) + dot16(left_low, high_ref[:, lo:], 0, 0)
        outs[s][...] = grams[s][...] + (small + dot16(left_high, high_ref[:, lo:], 0, 0))


def rays_gram(grams, parts, block):
    rows, width = parts[0].shape
    return pl.pallas_call(
        functools.partial(rays_kernel, block, len(grams), len(parts)),
        out_shape=[jax.ShapeDtypeStruct(g.shape, f32) for g in grams],
        in_specs=[pl.BlockSpec(memory_space=pltpu.VMEM)] * (len(grams) + len(parts)),
        out_specs=[pl.BlockSpec(memory_space=pltpu.VMEM)] * len(grams),
        scratch_shapes=[pltpu.VMEM((rows * len(parts), width), jnp.bfloat16)] * 2,
        compiler_params=pltpu.CompilerParams(vmem_limit_bytes=48 << 20),
        cost_estimate=cost(5),
        name="rays_gram",
    )(*grams, *parts)


AXES = ("front", "sub")


def leader_of(front, subs):
    return (subs // 2 - 1 + front % 2) % subs


def to_leader(x, fronts, subs):
    parts = [x]
    for j in range(subs - 1):
        pairs = []
        for f in range(fronts):
            leader = leader_of(f, subs)
            near = sorted((s for s in range(subs) if s != leader), key=lambda s: (abs(s - leader), s))
            pairs.append((f * subs + near[j], f * subs + leader))
        parts.append(lax.ppermute(x, AXES, pairs))
    return parts


def from_leader(x, owner, fronts, subs):
    pairs = [(f * subs + leader_of(f, subs), f * subs + owner) for f in range(fronts)]
    return lax.ppermute(x, AXES, pairs)


def local(row_values, front_of_row, child_factors, child_columns, damping):
    fronts, subs = lax.axis_size("front"), lax.axis_size("sub")
    width = row_values.shape[1]
    block = width // subs
    kid_parts = to_leader(child_factors, fronts, subs)
    outgoing = route(row_values, front_of_row, fronts)
    received = lax.all_to_all(outgoing, "front", split_axis=0, concat_axis=0, tiled=True)
    ray_parts = to_leader(received, fronts, subs)
    grams = children_gram(kid_parts, child_columns, damping, ray_parts[0], block)
    grams = rays_gram(grams, ray_parts[1:], block)
    factors, own = [], None
    for s in range(subs):
        factors.append(chol_block(grams[s], factors))
        sent = from_leader(factors[s], s, fronts, subs)
        sent = jnp.pad(sent, ((0, 0), (s * block, 0)))
        own = sent if own is None else own + sent
    return own[None]


def solution(mesh):
    in_specs = (
        P(("front", "sub"), None),
        P(("front", "sub"), None),
        P("front", "sub", None),
        P("front", None),
        P("front", None),
    )
    out_specs = P("front", "sub", None)
    return jax.shard_map(local, mesh=mesh, in_specs=in_specs, out_specs=out_specs, check_vma=False)
```

```python
import functools

import jax
import jax.numpy as jnp
from jax import lax
from jax.experimental import pallas as pl
from jax.experimental.pallas import tpu as pltpu
from jax.sharding import PartitionSpec as P


HIGHEST = lax.Precision.HIGHEST


def cost(us):
    return pl.CostEstimate(flops=int(us * 5e8), bytes_accessed=0, transcendentals=0)


f32 = jnp.float32


def dot(a, b, ca=1, cb=0):
    return lax.dot_general(a, b, (((ca,), (cb,)), ((), ())), precision=HIGHEST, preferred_element_type=f32)


def rowb(v, j):
    return jnp.broadcast_to(v[j:j + 1, :], v.shape)


def factor_tile(x, store_r, store_w, spread_ref, n=128, width=16):
    lane = lax.broadcasted_iota(jnp.int32, (8, n), 1)
    sub = lax.broadcasted_iota(jnp.int32, (8, n), 0)
    lane1 = lax.broadcasted_iota(jnp.int32, (1, n), 1)
    per = width // 8
    blocks = n // width

    def spread(v, c, slot):
        spread_ref[slot] = jnp.broadcast_to(v[:, c:c + 1], v.shape)
        return spread_ref[slot]

    own = [x[8 * v:8 * v + 8, :] for v in range(per)]
    nxt = [x[width + 8 * v:width + 8 * v + 8, :] for v in range(per)]
    rest = x[2 * width:, :]
    for blk in range(blocks):
        lo = blk * width
        base = (blk % 2) * 2 * per * width
        t = list(own)
        w = [jnp.where(lane < lo, own[v], jnp.where(lane == sub + (lo + 8 * v), 1.0, 0.0)) for v in range(per)]
        b = [[None] * width for _ in range(per)]
        for c in range(width):
            for v in range(per):
                b[v][c] = spread(own[v], lo + c, base + v * width + c)
        last = blk == blocks - 1
        if not last:
            later = [[None] * width for _ in range(per)]
            for c in range(width):
                for v in range(per):
                    later[v][c] = spread(nxt[v], lo + c, base + (per + v) * width + c)
        for j in range(width):
            pv, jj = divmod(j, 8)
            here = sub == jj
            d = rowb(b[pv][j], jj)
            inv = 1.0 / d
            root = lax.rsqrt(d)
            cols = [b[v][j] for v in range(per)]
            cols[pv] = jnp.where(here, -1.0, cols[pv])
            for c in range(j + 1, width):
                row = rowb(b[pv][c], jj)
                if c == j + 1:
                    for v in range(per):
                        kept = jnp.where(here, 0.0, b[v][c]) if v == pv else b[v][c]
                        b[v][c] = kept - (cols[v] * row) * inv
                else:
                    row = row * inv
                    for v in range(per):
                        kept = jnp.where(here, 0.0, b[v][c]) if v == pv else b[v][c]
                        b[v][c] = kept - cols[v] * row
            trow, wrow = rowb(t[pv], jj), rowb(w[pv], jj)
            store_r(lo + j, jnp.where(lane1 >= lo + j, (trow * root)[0:1], 0.0))
            store_w(lo + j, (wrow * root)[0:1])
            tp, wp = trow * inv, wrow * inv
            for v in range(per):
                if last and v < pv:
                    continue
                for a, p in ((t, tp), (w, wp)):
                    kept = jnp.where(here, 0.0, a[v]) if v == pv else a[v]
                    a[v] = kept - cols[v] * p
        if last:
            break
        inside = (lane >= lo) & (lane < lo + width)
        z = [jnp.where(lane < lo + width, w[v], t[v]) for v in range(per)]
        new = []
        for v in range(per):
            terms = [later[v][c] * rowb(z[c // 8], c % 8) for c in range(width)]
            while len(terms) > 1:
                terms = [terms[q] + terms[q + 1] for q in range(0, len(terms), 2)]
            new.append(jnp.where(inside, 0.0, nxt[v]) - terms[0])
        own = new
        if rest.shape[0]:
            parts = [jnp.zeros((lo, n), f32)] if lo else []
            parts += z + [jnp.zeros((n - lo - width, n), f32)]
            zpad = jnp.concatenate(parts, axis=0)
            lane_r = lax.broadcasted_iota(jnp.int32, rest.shape, 1)
            rest = jnp.where((lane_r >= lo) & (lane_r < lo + width), 0.0, rest) - dot(rest, zpad)
            nxt = [rest[8 * v:8 * v + 8, :] for v in range(per)]
            rest = rest[width:, :]


def block_kernel(nprev, width, *refs):
    g_ref = refs[0]
    prev = refs[1:1 + nprev]
    r_ref, tile_ref, w_ref, spread_ref = refs[1 + nprev:]
    rows, cols = g_ref.shape
    half = w_ref.shape[0]
    u = g_ref[...]
    for t in range(nprev):
        off = rows * (nprev - t)
        u = u - dot(prev[t][:, off:off + rows], prev[t][:, off:], 0, 0)
    r_ref[...] = u

    def store_r(i, v):
        tile_ref[i:i + 1, :] = v

    def store_w(i, v):
        w_ref[i:i + 1, :] = v

    def panel(p, carry):
        for q in range(1, rows // half):

            @pl.when(p == q)
            def _():
                a = q * half
                done = dot(r_ref[0:a, a:a + half], r_ref[0:a, a:], 0, 0)
                r_ref[a:a + half, a:] = r_ref[a:a + half, a:] - done

        at = pl.ds(pl.multiple_of(p * half, half), half)
        factor_tile(r_ref[at, at], store_r, store_w, spread_ref, half, width)
        for q in range(rows // half):

            @pl.when(p == q)
            def _():
                a = q * half
                if a:
                    r_ref[a:a + half, 0:a] = jnp.zeros((half, a), f32)
                if a + half < cols:
                    r_ref[a:a + half, a + half:] = dot(w_ref[...], r_ref[a:a + half, a + half:])
                r_ref[a:a + half, a:a + half] = tile_ref[...]

        return carry

    lax.fori_loop(0, rows // half, panel, 0)


def chol_block(g, prev, width=16):
    n = len(prev)
    return pl.pallas_call(
        functools.partial(block_kernel, n, width),
        out_shape=jax.ShapeDtypeStruct(g.shape, f32),
        in_specs=[pl.BlockSpec(memory_space=pltpu.VMEM)] * (n + 1),
        out_specs=pl.BlockSpec(memory_space=pltpu.VMEM),
        scratch_shapes=[
            pltpu.VMEM((128, 128), f32),
            pltpu.VMEM((128, 128), f32),
            pltpu.VMEM((width * width // 2, 8, 128), f32),
        ],
        compiler_params=pltpu.CompilerParams(vmem_limit_bytes=12 << 20),
        cost_estimate=cost(6),
        name="factor_block",
    )(g, *prev)


def split3(x):
    high = x.astype(jnp.bfloat16)
    rest = x - high.astype(f32)
    mid = rest.astype(jnp.bfloat16)
    low = (rest - mid.astype(f32)).astype(jnp.bfloat16)
    return high, mid, low


def pick_exact(onehot, x, ca, cb, onehot_left):
    total = None
    for piece in split3(x):
        a, b = (onehot, piece) if onehot_left else (piece, onehot)
        part = lax.dot_general(a, b, (((ca,), (cb,)), ((), ())), preferred_element_type=f32)
        total = part if total is None else total + part
    return total


def route_kernel(capacity, rows_ref, row_ref, out_ref):
    n = rows_ref.shape[0]
    slots = out_ref.shape[0]
    down = lax.broadcasted_iota(jnp.int32, (n, n), 0)
    across = lax.broadcasted_iota(jnp.int32, (n, n), 1)
    row = row_ref[...].astype(f32)
    column = jnp.sum(jnp.where(down == across, jnp.broadcast_to(row, (n, n)), 0.0), axis=1, keepdims=True)
    earlier = (column == row) & (down < across)
    position = jnp.sum(jnp.where(earlier, 1.0, 0.0), axis=0, keepdims=True)
    slot = row_ref[...] * capacity + position.astype(jnp.int32)
    pick = lax.broadcasted_iota(jnp.int32, (slots, n), 0) == slot
    out_ref[...] = pick_exact(pick.astype(f32).astype(jnp.bfloat16), rows_ref[...], 1, 0, True)


def route(row_values, front_of_row, fronts):
    n, width = row_values.shape
    capacity = 2 * n // fronts
    return pl.pallas_call(
        functools.partial(route_kernel, capacity),
        out_shape=jax.ShapeDtypeStruct((fronts * capacity, width), f32),
        in_specs=[pl.BlockSpec(memory_space=pltpu.VMEM)] * 2,
        out_specs=pl.BlockSpec(memory_space=pltpu.VMEM),
        cost_estimate=cost(3),
        name="route",
    )(row_values, front_of_row.reshape(1, n))


def dot16(a, b, ca, cb):
    return lax.dot_general(a, b, (((ca,), (cb,)), ((), ())), preferred_element_type=f32)


def split2(x):
    high = x.astype(jnp.bfloat16)
    return high, (x - high.astype(f32)).astype(jnp.bfloat16)


def gram_block(high_ref, low_ref, lo, block):
    left_high, left_low = high_ref[:, lo:lo + block], low_ref[:, lo:lo + block]
    small = dot16(left_high, low_ref[:, lo:], 0, 0) + dot16(left_low, high_ref[:, lo:], 0, 0)
    return small + dot16(left_high, high_ref[:, lo:], 0, 0)


def children_kernel(block, nparts, *refs):
    parts = refs[:nparts]
    columns_ref, damping_ref, own_ref = refs[nparts:nparts + 3]
    outs = refs[nparts + 3:-3]
    stack_ref, high_ref, low_ref = refs[-3:]
    width = high_ref.shape[1]
    kids, rows, contrib = parts[0].shape
    each = rows * nparts
    for q in range(nparts):
        stack_ref[:, q * rows:(q + 1) * rows, :] = parts[q][...]
    high_ref[kids * each:, :], low_ref[kids * each:, :] = split2(own_ref[...])
    parent = lax.broadcasted_iota(jnp.int32, (width, contrib), 0)

    def place(c, carry):
        spread = (parent == columns_ref[pl.ds(c, 1), :]).astype(f32).astype(jnp.bfloat16)
        high, low = split2(stack_ref[c])
        at = pl.ds(pl.multiple_of(c * each, each), each)
        high_ref[at, :] = dot16(high, spread, 1, 1).astype(jnp.bfloat16)
        low_ref[at, :] = dot16(low, spread, 1, 1).astype(jnp.bfloat16)
        return carry

    lax.fori_loop(0, kids, place, 0)
    weight = damping_ref[...]
    for s, out_ref in enumerate(outs):
        lo = s * block
        down = lax.broadcasted_iota(jnp.int32, out_ref.shape, 0)
        across = lax.broadcasted_iota(jnp.int32, out_ref.shape, 1)
        diag = jnp.where(down == across, weight[:, lo:] * weight[:, lo:], 0.0)
        out_ref[...] = diag + gram_block(high_ref, low_ref, lo, block)


def block_shapes(width, block):
    return [jax.ShapeDtypeStruct((block, width - lo), f32) for lo in range(0, width, block)]


def children_gram(parts, columns, damping, own, block):
    width = damping.shape[1]
    kids, rows, contrib = parts[0].shape
    shapes = block_shapes(width, block)
    return pl.pallas_call(
        functools.partial(children_kernel, block, len(parts)),
        out_shape=shapes,
        in_specs=[pl.BlockSpec(memory_space=pltpu.VMEM)] * (len(parts) + 3),
        out_specs=[pl.BlockSpec(memory_space=pltpu.VMEM)] * len(shapes),
        scratch_shapes=[pltpu.VMEM((kids, rows * len(parts), contrib), f32)]
        + [pltpu.VMEM((kids * rows * len(parts) + own.shape[0], width), jnp.bfloat16)] * 2,
        compiler_params=pltpu.CompilerParams(vmem_limit_bytes=28 << 20),
        cost_estimate=cost(10),
        name="children_gram",
    )(*parts, columns, damping, own)


def rays_kernel(block, nblocks, nparts, *refs):
    grams = refs[:nblocks]
    parts = refs[nblocks:nblocks + nparts]
    outs = refs[nblocks + nparts:-2]
    high_ref, low_ref = refs[-2:]
    rows = parts[0].shape[0]
    for q, part in enumerate(parts):
        at = slice(q * rows, (q + 1) * rows)
        high_ref[at, :], low_ref[at, :] = split2(part[...])
    for s in range(nblocks):
        lo = s * block
        outs[s][...] = grams[s][...] + gram_block(high_ref, low_ref, lo, block)


def rays_gram(grams, parts, block):
    rows, width = parts[0].shape
    return pl.pallas_call(
        functools.partial(rays_kernel, block, len(grams), len(parts)),
        out_shape=[jax.ShapeDtypeStruct(g.shape, f32) for g in grams],
        in_specs=[pl.BlockSpec(memory_space=pltpu.VMEM)] * (len(grams) + len(parts)),
        out_specs=[pl.BlockSpec(memory_space=pltpu.VMEM)] * len(grams),
        scratch_shapes=[pltpu.VMEM((rows * len(parts), width), jnp.bfloat16)] * 2,
        compiler_params=pltpu.CompilerParams(vmem_limit_bytes=20 << 20),
        cost_estimate=cost(5),
        name="rays_gram",
    )(*grams, *parts)


AXES = ("front", "sub")


def leader_of(front, subs):
    return (subs // 2 - 1 + front % 2) % subs


def to_leader(x, fronts, subs):
    parts = [x]
    for j in range(subs - 1):
        pairs = []
        for f in range(fronts):
            leader = leader_of(f, subs)
            near = sorted((s for s in range(subs) if s != leader), key=lambda s: (abs(s - leader), s))
            pairs.append((f * subs + near[j], f * subs + leader))
        parts.append(lax.ppermute(x, AXES, pairs))
    return parts


def from_leader(x, owner, fronts, subs):
    pairs = [(f * subs + leader_of(f, subs), f * subs + owner) for f in range(fronts)]
    return lax.ppermute(x, AXES, pairs)


def local(row_values, front_of_row, child_factors, child_columns, damping):
    fronts, subs = lax.axis_size("front"), lax.axis_size("sub")
    width = row_values.shape[1]
    block = width // subs
    kid_parts = to_leader(child_factors, fronts, subs)
    outgoing = route(row_values, front_of_row, fronts)
    received = lax.all_to_all(outgoing, "front", split_axis=0, concat_axis=0, tiled=True)
    ray_parts = to_leader(received, fronts, subs)
    grams = children_gram(kid_parts, child_columns, damping, ray_parts[0], block)
    grams = rays_gram(grams, ray_parts[1:], block)
    factors, own = [], None
    for s in range(subs):
        factors.append(chol_block(grams[s], factors))
        sent = from_leader(factors[s], s, fronts, subs)
        sent = jnp.pad(sent, ((0, 0), (s * block, 0)))
        own = sent if own is None else own + sent
    return own[None]


def solution(mesh):
    in_specs = (
        P(("front", "sub"), None),
        P(("front", "sub"), None),
        P("front", "sub", None),
        P("front", None),
        P("front", None),
    )
    out_specs = P("front", "sub", None)

    return jax.shard_map(local, mesh=mesh, in_specs=in_specs, out_specs=out_specs, check_vma=False)
```

```python
import functools

import jax
import jax.numpy as jnp
from jax import lax
from jax.experimental import pallas as pl
from jax.experimental.pallas import tpu as pltpu
from jax.sharding import PartitionSpec as P


HIGHEST = lax.Precision.HIGHEST
TILE = 128
AXES = ("front", "sub")


def cost(us):
    return pl.CostEstimate(flops=int(us * 5e8), bytes_accessed=0, transcendentals=0)


f32 = jnp.float32


def leader_of(front, subs):
    return (subs // 2 - 1 + front % 2) % subs


def on_leader(body, *refs):
    @pl.when(lax.axis_index("sub") == leader_of(lax.axis_index("front"), lax.axis_size("sub")))
    def _():
        body(*refs)


def dot(a, b, ca=1, cb=0):
    return lax.dot_general(a, b, (((ca,), (cb,)), ((), ())), precision=HIGHEST, preferred_element_type=f32)


def dot16(a, b, ca, cb):
    return lax.dot_general(a, b, (((ca,), (cb,)), ((), ())), preferred_element_type=f32)


def split2(x):
    high = x.astype(jnp.bfloat16)
    return high, (x - high.astype(f32)).astype(jnp.bfloat16)


def pair_dot(a, b, ca, cb):
    small = dot16(a[0], b[1], ca, cb) + dot16(a[1], b[0], ca, cb)
    return small + dot16(a[0], b[0], ca, cb)


def dot3(a, b, ca=1, cb=0):
    return pair_dot(split2(a), split2(b), ca, cb)


def rowb(v, j):
    return jnp.broadcast_to(v[j:j + 1, :], v.shape)


def factor_tile(x, store_r, store_w, spread_ref, n=128, width=16):
    lane = lax.broadcasted_iota(jnp.int32, (8, n), 1)
    sub = lax.broadcasted_iota(jnp.int32, (8, n), 0)
    lane1 = lax.broadcasted_iota(jnp.int32, (1, n), 1)
    per = width // 8
    blocks = n // width

    def spread(v, c, slot):
        spread_ref[slot] = jnp.broadcast_to(v[:, c:c + 1], v.shape)
        return spread_ref[slot]

    own = [x[8 * v:8 * v + 8, :] for v in range(per)]
    nxt = [x[width + 8 * v:width + 8 * v + 8, :] for v in range(per)]
    rest = x[2 * width:, :]
    for blk in range(blocks):
        lo = blk * width
        base = (blk % 2) * 2 * per * width
        t = list(own)
        w = [jnp.where(lane < lo, own[v], jnp.where(lane == sub + (lo + 8 * v), 1.0, 0.0)) for v in range(per)]
        b = [[None] * width for _ in range(per)]
        for c in range(width):
            for v in range(per):
                b[v][c] = spread(own[v], lo + c, base + v * width + c)
        last = blk == blocks - 1
        if not last:
            later = [[None] * width for _ in range(per)]
            for c in range(width):
                for v in range(per):
                    later[v][c] = spread(nxt[v], lo + c, base + (per + v) * width + c)
        for j in range(width):
            pv, jj = divmod(j, 8)
            here = sub == jj
            d = rowb(b[pv][j], jj)
            inv = 1.0 / d
            root = lax.rsqrt(d)
            cols = [b[v][j] for v in range(per)]
            cols[pv] = jnp.where(here, -1.0, cols[pv])
            for c in range(j + 1, width):
                row = rowb(b[pv][c], jj)
                if c == j + 1:
                    for v in range(per):
                        kept = jnp.where(here, 0.0, b[v][c]) if v == pv else b[v][c]
                        b[v][c] = kept - (cols[v] * row) * inv
                else:
                    row = row * inv
                    for v in range(per):
                        kept = jnp.where(here, 0.0, b[v][c]) if v == pv else b[v][c]
                        b[v][c] = kept - cols[v] * row
            trow, wrow = rowb(t[pv], jj), rowb(w[pv], jj)
            store_r(lo + j, jnp.where(lane1 >= lo + j, (trow * root)[0:1], 0.0))
            store_w(lo + j, (wrow * root)[0:1])
            tp, wp = trow * inv, wrow * inv
            for v in range(per):
                if last and v < pv:
                    continue
                for a, p in ((t, tp), (w, wp)):
                    kept = jnp.where(here, 0.0, a[v]) if v == pv else a[v]
                    a[v] = kept - cols[v] * p
        if last:
            break
        inside = (lane >= lo) & (lane < lo + width)
        z = [jnp.where(lane < lo + width, w[v], t[v]) for v in range(per)]
        new = []
        for v in range(per):
            terms = [later[v][c] * rowb(z[c // 8], c % 8) for c in range(width)]
            while len(terms) > 1:
                terms = [terms[q] + terms[q + 1] for q in range(0, len(terms), 2)]
            new.append(jnp.where(inside, 0.0, nxt[v]) - terms[0])
        own = new
        if rest.shape[0]:
            parts = [jnp.zeros((lo, n), f32)] if lo else []
            parts += z + [jnp.zeros((n - lo - width, n), f32)]
            zpad = jnp.concatenate(parts, axis=0)
            lane_r = lax.broadcasted_iota(jnp.int32, rest.shape, 1)
            rest = jnp.where((lane_r >= lo) & (lane_r < lo + width), 0.0, rest) - dot(rest, zpad)
            nxt = [rest[8 * v:8 * v + 8, :] for v in range(per)]
            rest = rest[width:, :]


def factor_loop(r_ref, tile_ref, w_ref, spread_ref, width, keep=None):
    rows, cols = r_ref.shape
    half = w_ref.shape[0]

    def store_r(i, v):
        tile_ref[i:i + 1, :] = v

    def store_w(i, v):
        w_ref[i:i + 1, :] = v

    def panel(p, carry):
        for q in range(1, rows // half):

            @pl.when(p == q)
            def _():
                a = q * half
                done = dot3(r_ref[0:a, a:a + half], r_ref[0:a, a:], 0, 0)
                r_ref[a:a + half, a:] = r_ref[a:a + half, a:] - done

        at = pl.ds(pl.multiple_of(p * half, half), half)
        factor_tile(r_ref[at, at], store_r, store_w, spread_ref, half, width)
        if keep is not None:
            keep[at, :] = w_ref[...]
        for q in range(rows // half):

            @pl.when(p == q)
            def _():
                a = q * half
                if a:
                    r_ref[a:a + half, 0:a] = jnp.zeros((half, a), f32)
                if a + half < cols:
                    r_ref[a:a + half, a + half:] = dot3(w_ref[...], r_ref[a:a + half, a + half:])
                r_ref[a:a + half, a:a + half] = tile_ref[...]

        return carry

    lax.fori_loop(0, rows // half, panel, 0)


def block_kernel(nprev, width, *refs):
    g_ref = refs[0]
    prev = refs[1:1 + nprev]
    r_ref = refs[1 + nprev]
    rows = g_ref.shape[0]
    u = g_ref[...]
    for t in range(nprev):
        off = rows * (nprev - t)
        u = u - dot3(prev[t][:, off:off + rows], prev[t][:, off:], 0, 0)
    r_ref[...] = u
    factor_loop(*refs[1 + nprev:], width)


def factor_scratch(width):
    return [
        pltpu.VMEM((TILE, TILE), f32),
        pltpu.VMEM((TILE, TILE), f32),
        pltpu.VMEM((width * width // 2, 8, TILE), f32),
    ]


def chol_block(g, prev, width=16):
    n = len(prev)
    return pl.pallas_call(
        functools.partial(on_leader, functools.partial(block_kernel, n, width)),
        out_shape=jax.ShapeDtypeStruct(g.shape, f32),
        in_specs=[pl.BlockSpec(memory_space=pltpu.VMEM)] * (n + 1),
        out_specs=pl.BlockSpec(memory_space=pltpu.VMEM),
        scratch_shapes=factor_scratch(width),
        compiler_params=pltpu.CompilerParams(vmem_limit_bytes=12 << 20),
        cost_estimate=cost(6),
        name="factor_block",
    )(g, *prev)


def split3(x):
    high = x.astype(jnp.bfloat16)
    rest = x - high.astype(f32)
    mid = rest.astype(jnp.bfloat16)
    low = (rest - mid.astype(f32)).astype(jnp.bfloat16)
    return high, mid, low


def pick_exact(onehot, x, ca, cb, onehot_left):
    total = None
    for piece in split3(x):
        a, b = (onehot, piece) if onehot_left else (piece, onehot)
        part = lax.dot_general(a, b, (((ca,), (cb,)), ((), ())), preferred_element_type=f32)
        total = part if total is None else total + part
    return total


def route_kernel(capacity, rows_ref, row_ref, *out_refs):
    n = rows_ref.shape[0]
    slots, width = out_refs[0].shape
    down = lax.broadcasted_iota(jnp.int32, (n, n), 0)
    across = lax.broadcasted_iota(jnp.int32, (n, n), 1)
    row = row_ref[...].astype(f32)
    column = jnp.sum(jnp.where(down == across, jnp.broadcast_to(row, (n, n)), 0.0), axis=1, keepdims=True)
    earlier = (column == row) & (down < across)
    position = jnp.sum(jnp.where(earlier, 1.0, 0.0), axis=0, keepdims=True)
    slot = row_ref[...] * capacity + position.astype(jnp.int32)
    pick = lax.broadcasted_iota(jnp.int32, (slots, n), 0) == slot
    pick = pick.astype(f32).astype(jnp.bfloat16)
    for h, out_ref in enumerate(out_refs):
        out_ref[...] = pick_exact(pick, rows_ref[:, h * width:(h + 1) * width], 1, 0, True)


def route(row_values, front_of_row, fronts):
    n, width = row_values.shape
    capacity = 2 * n // fronts
    return pl.pallas_call(
        functools.partial(route_kernel, capacity),
        out_shape=[jax.ShapeDtypeStruct((fronts * capacity, width // 2), f32)] * 2,
        in_specs=[pl.BlockSpec(memory_space=pltpu.VMEM)] * 2,
        out_specs=[pl.BlockSpec(memory_space=pltpu.VMEM)] * 2,
        cost_estimate=cost(3),
        name="route",
    )(row_values, front_of_row.reshape(1, n))


def gram_block(high_ref, low_ref, lo, block):
    left = high_ref[:, lo:lo + block], low_ref[:, lo:lo + block]
    return pair_dot(left, (high_ref[:, lo:], low_ref[:, lo:]), 0, 0)


def children_kernel(block, nparts, *refs):
    parts = refs[:nparts]
    columns_ref, damping_ref = refs[nparts:nparts + 2]
    outs = refs[nparts + 2:-3]
    stack_ref, high_ref, low_ref = refs[-3:]
    width = high_ref.shape[1]
    kids, rows, contrib = parts[0].shape
    each = rows * nparts
    for q in range(nparts):
        stack_ref[:, q * rows:(q + 1) * rows, :] = parts[q][...]
    parent = lax.broadcasted_iota(jnp.int32, (width, contrib), 0)

    def place(c, carry):
        spread = (parent == columns_ref[pl.ds(c, 1), :]).astype(f32).astype(jnp.bfloat16)
        high, low = split2(stack_ref[c])
        at = pl.ds(pl.multiple_of(c * each, each), each)
        high_ref[at, :] = dot16(high, spread, 1, 1).astype(jnp.bfloat16)
        low_ref[at, :] = dot16(low, spread, 1, 1).astype(jnp.bfloat16)
        return carry

    lax.fori_loop(0, kids, place, 0)
    weight = damping_ref[...]
    for s, out_ref in enumerate(outs):
        lo = s * block
        down = lax.broadcasted_iota(jnp.int32, out_ref.shape, 0)
        across = lax.broadcasted_iota(jnp.int32, out_ref.shape, 1)
        diag = jnp.where(down == across, weight[:, lo:] * weight[:, lo:], 0.0)
        out_ref[...] = diag + gram_block(high_ref, low_ref, lo, block)


def block_shapes(width, block):
    return [jax.ShapeDtypeStruct((block, width - lo), f32) for lo in range(0, width, block)]


def children_gram(parts, columns, damping, block):
    width = damping.shape[1]
    kids, rows, contrib = parts[0].shape
    shapes = block_shapes(width, block)
    return pl.pallas_call(
        functools.partial(on_leader, functools.partial(children_kernel, block, len(parts))),
        out_shape=shapes,
        in_specs=[pl.BlockSpec(memory_space=pltpu.VMEM)] * (len(parts) + 2),
        out_specs=[pl.BlockSpec(memory_space=pltpu.VMEM)] * len(shapes),
        scratch_shapes=[pltpu.VMEM((kids, rows * len(parts), contrib), f32)]
        + [pltpu.VMEM((kids * rows * len(parts), width), jnp.bfloat16)] * 2,
        compiler_params=pltpu.CompilerParams(vmem_limit_bytes=28 << 20),
        cost_estimate=cost(10),
        name="children_gram",
    )(*parts, columns, damping)


def split_parts(parts, high_ref, low_ref):
    rows = parts[0].shape[0]
    for q, part in enumerate(parts):
        at = slice(q * rows, (q + 1) * rows)
        high_ref[at, :], low_ref[at, :] = split2(part[...])


def lead_kernel(nlead, nparts, width, *refs):
    grams = refs[:nlead]
    parts = refs[nlead:nlead + nparts]
    lead_ref, top_ref, keep_ref, high_ref, low_ref = refs[nlead + nparts:nlead + nparts + 5]
    scratch = refs[nlead + nparts + 5:]
    block = grams[0].shape[0]
    cols = lead_ref.shape[1]
    split_parts(parts, high_ref, low_ref)
    for s in range(nlead):
        lo = s * block
        lead_ref[lo:lo + block, lo:] = grams[s][:, 0:cols - lo] + gram_block(high_ref, low_ref, lo, block)
    factor_loop(lead_ref, *scratch, width, keep_ref)
    top_ref[...] = lead_ref[0:block, :]


def lead_factor(grams, parts, width=16):
    block = grams[0].shape[0]
    rows, cols = parts[0].shape
    nlead = cols // block
    ins = [*grams[:nlead], *parts]
    return pl.pallas_call(
        functools.partial(on_leader, functools.partial(lead_kernel, nlead, len(parts), width)),
        out_shape=[
            jax.ShapeDtypeStruct((cols, cols), f32),
            jax.ShapeDtypeStruct((block, cols), f32),
            jax.ShapeDtypeStruct((cols, TILE), f32),
            jax.ShapeDtypeStruct((rows * len(parts), cols), jnp.bfloat16),
            jax.ShapeDtypeStruct((rows * len(parts), cols), jnp.bfloat16),
        ],
        in_specs=[pl.BlockSpec(memory_space=pltpu.VMEM)] * len(ins),
        out_specs=[pl.BlockSpec(memory_space=pltpu.VMEM)] * 5,
        scratch_shapes=factor_scratch(width),
        compiler_params=pltpu.CompilerParams(vmem_limit_bytes=20 << 20),
        cost_estimate=cost(14),
        name="lead_factor",
    )(*ins)


def cross_kernel(nblocks, nlead, nparts, *refs):
    grams = refs[:nblocks]
    parts = refs[nblocks:nblocks + nparts]
    lead_ref, keep_ref, high1_ref, low1_ref = refs[nblocks + nparts:nblocks + nparts + 4]
    outs = refs[nblocks + nparts + 4:-3]
    x_ref, high_ref, low_ref = refs[-3:]
    block = grams[0].shape[0]
    cols = lead_ref.shape[1]
    split_parts(parts, high_ref, low_ref)
    right = high_ref[...], low_ref[...]
    for s in range(nlead):
        at = slice(s * block, (s + 1) * block)
        left = high1_ref[:, at], low1_ref[:, at]
        x_ref[at, :] = grams[s][:, cols - s * block:] + pair_dot(left, right, 0, 0)
    for a in range(0, cols, TILE):
        at = slice(a, a + TILE)
        u = x_ref[at, :]
        if a:
            u = u - dot3(lead_ref[0:a, at], x_ref[0:a, :], 0, 0)
        x_ref[at, :] = dot3(keep_ref[at, :], u)
    for s in range(nlead):
        at = slice(s * block, (s + 1) * block)
        if s:
            outs[s][:, 0:cols - s * block] = lead_ref[at, s * block:]
            outs[s][:, cols - s * block:] = x_ref[at, :]
        else:
            outs[s][...] = x_ref[at, :]
    high1, low1 = split2(x_ref[...])
    for s in range(nlead, nblocks):
        lo = (s - nlead) * block
        left = high1[:, lo:lo + block], low1[:, lo:lo + block]
        done = pair_dot(left, (high1[:, lo:], low1[:, lo:]), 0, 0)
        outs[s][...] = grams[s][...] + gram_block(high_ref, low_ref, lo, block) - done


def cross_update(grams, parts, lead, keep, high1, low1):
    block = grams[0].shape[0]
    rows, cols = parts[0].shape
    nlead = cols // block
    ins = [*grams, *parts, lead, keep, high1, low1]
    shapes = [jax.ShapeDtypeStruct(g.shape, f32) for g in grams]
    shapes[0] = jax.ShapeDtypeStruct((block, grams[0].shape[1] - cols), f32)
    tall = (rows * len(parts), cols)
    return pl.pallas_call(
        functools.partial(on_leader, functools.partial(cross_kernel, len(grams), nlead, len(parts))),
        out_shape=shapes,
        in_specs=[pl.BlockSpec(memory_space=pltpu.VMEM)] * len(ins),
        out_specs=[pl.BlockSpec(memory_space=pltpu.VMEM)] * len(shapes),
        scratch_shapes=[pltpu.VMEM((cols, cols), f32)] + [pltpu.VMEM(tall, jnp.bfloat16)] * 2,
        compiler_params=pltpu.CompilerParams(vmem_limit_bytes=28 << 20),
        cost_estimate=cost(9),
        name="cross_update",
    )(*ins)


def to_leader(x, fronts, subs):
    parts = [x]
    for j in range(subs - 1):
        pairs = []
        for f in range(fronts):
            leader = leader_of(f, subs)
            near = sorted((s for s in range(subs) if s != leader), key=lambda s: (abs(s - leader), s))
            pairs.append((f * subs + near[j], f * subs + leader))
        parts.append(lax.ppermute(x, AXES, pairs))
    return parts


def from_leader(x, owner, fronts, subs):
    pairs = [(f * subs + leader_of(f, subs), f * subs + owner) for f in range(fronts)]
    return lax.ppermute(x, AXES, pairs)


def local(row_values, front_of_row, child_factors, child_columns, damping):
    fronts, subs = lax.axis_size("front"), lax.axis_size("sub")
    width = row_values.shape[1]
    block = width // subs
    kid_parts = to_leader(child_factors, fronts, subs)
    halves = []
    for outgoing in route(row_values, front_of_row, fronts):
        received = lax.all_to_all(outgoing, "front", split_axis=0, concat_axis=0, tiled=True)
        halves.append(to_leader(received, fronts, subs))
    grams = children_gram(kid_parts, child_columns, damping, block)
    lead, top, keep, high1, low1 = lead_factor(grams, halves[0])
    pieces = []

    def send(x, owner, at):
        sent = from_leader(x, owner, fronts, subs)
        pieces.append(jnp.pad(sent, ((0, 0), (at, width - at - x.shape[1]))))

    nlead = subs // 2
    send(top, 0, 0)
    rest = cross_update(grams, halves[1], lead, keep, high1, low1)
    send(rest[0], 0, nlead * block)
    for s in range(1, nlead):
        send(rest[s], s, s * block)
    factors = []
    for s in range(nlead, subs):
        factors.append(chol_block(rest[s], factors))
        send(factors[-1], s, s * block)
    return functools.reduce(jnp.add, pieces)[None]


def solution(mesh):
    in_specs = (
        P(("front", "sub"), None),
        P(("front", "sub"), None),
        P("front", "sub", None),
        P("front", None),
        P("front", None),
    )
    out_specs = P("front", "sub", None)

    return jax.shard_map(local, mesh=mesh, in_specs=in_specs, out_specs=out_specs, check_vma=False)
```

```python
import functools

import jax
import jax.numpy as jnp
from jax import lax
from jax.experimental import pallas as pl
from jax.experimental.pallas import tpu as pltpu
from jax.sharding import PartitionSpec as P


TILE = 128
AXES = ("front", "sub")


def cost(us):
    return pl.CostEstimate(flops=int(us * 5e8), bytes_accessed=0, transcendentals=0)


f32 = jnp.float32


def leader_of(front, subs):
    return (subs // 2 - 1 + front % 2) % subs


def on_leader(body, *refs):
    @pl.when(lax.axis_index("sub") == leader_of(lax.axis_index("front"), lax.axis_size("sub")))
    def _():
        body(*refs)


def dot16(a, b, ca, cb):
    return lax.dot_general(a, b, (((ca,), (cb,)), ((), ())), preferred_element_type=f32)


def split2(x):
    high = x.astype(jnp.bfloat16)
    return high, (x - high.astype(f32)).astype(jnp.bfloat16)


def pair_dot(a, b, ca, cb):
    small = dot16(a[0], b[1], ca, cb) + dot16(a[1], b[0], ca, cb)
    return small + dot16(a[0], b[0], ca, cb)


def dot3(a, b, ca=1, cb=0):
    return pair_dot(split2(a), split2(b), ca, cb)


def rowb(v, j):
    return jnp.broadcast_to(v[j:j + 1, :], v.shape)


def factor_tile(x, store_r, store_w, spread_ref, n=128, width=16):
    lane = lax.broadcasted_iota(jnp.int32, (8, n), 1)
    sub = lax.broadcasted_iota(jnp.int32, (8, n), 0)
    lane1 = lax.broadcasted_iota(jnp.int32, (1, n), 1)
    per = width // 8
    blocks = n // width

    def spread(v, c, slot):
        spread_ref[slot] = jnp.broadcast_to(v[:, c:c + 1], v.shape)
        return spread_ref[slot]

    own = [x[8 * v:8 * v + 8, :] for v in range(per)]
    nxt = [x[width + 8 * v:width + 8 * v + 8, :] for v in range(per)]
    rest = x[2 * width:, :]
    for blk in range(blocks):
        lo = blk * width
        base = (blk % 2) * 2 * per * width
        t = list(own)
        w = [jnp.where(lane < lo, own[v], jnp.where(lane == sub + (lo + 8 * v), 1.0, 0.0)) for v in range(per)]
        b = [[None] * width for _ in range(per)]
        for c in range(width):
            for v in range(per):
                b[v][c] = spread(own[v], lo + c, base + v * width + c)
        last = blk == blocks - 1
        if not last:
            later = [[None] * width for _ in range(per)]
            for c in range(width):
                for v in range(per):
                    later[v][c] = spread(nxt[v], lo + c, base + (per + v) * width + c)
        for j in range(width):
            pv, jj = divmod(j, 8)
            here = sub == jj
            d = rowb(b[pv][j], jj)
            inv = 1.0 / d
            root = lax.rsqrt(d)
            cols = [b[v][j] for v in range(per)]
            cols[pv] = jnp.where(here, -1.0, cols[pv])
            for c in range(j + 1, width):
                row = rowb(b[pv][c], jj)
                if c == j + 1:
                    for v in range(per):
                        kept = jnp.where(here, 0.0, b[v][c]) if v == pv else b[v][c]
                        b[v][c] = kept - (cols[v] * row) * inv
                else:
                    row = row * inv
                    for v in range(per):
                        kept = jnp.where(here, 0.0, b[v][c]) if v == pv else b[v][c]
                        b[v][c] = kept - cols[v] * row
            trow, wrow = rowb(t[pv], jj), rowb(w[pv], jj)
            store_r(lo + j, jnp.where(lane1 >= lo + j, (trow * root)[0:1], 0.0))
            store_w(lo + j, (wrow * root)[0:1])
            tp, wp = trow * inv, wrow * inv
            for v in range(per):
                if last and v < pv:
                    continue
                for a, p in ((t, tp), (w, wp)):
                    kept = jnp.where(here, 0.0, a[v]) if v == pv else a[v]
                    a[v] = kept - cols[v] * p
        if last:
            break
        inside = (lane >= lo) & (lane < lo + width)
        z = [jnp.where(lane < lo + width, w[v], t[v]) for v in range(per)]
        new = []
        for v in range(per):
            terms = [later[v][c] * rowb(z[c // 8], c % 8) for c in range(width)]
            while len(terms) > 1:
                terms = [terms[q] + terms[q + 1] for q in range(0, len(terms), 2)]
            new.append(jnp.where(inside, 0.0, nxt[v]) - terms[0])
        own = new
        if rest.shape[0]:
            parts = [jnp.zeros((lo, n), f32)] if lo else []
            parts += z + [jnp.zeros((n - lo - width, n), f32)]
            zpad = jnp.concatenate(parts, axis=0)
            lane_r = lax.broadcasted_iota(jnp.int32, rest.shape, 1)
            rest = jnp.where((lane_r >= lo) & (lane_r < lo + width), 0.0, rest) - dot3(rest, zpad)
            nxt = [rest[8 * v:8 * v + 8, :] for v in range(per)]
            rest = rest[width:, :]


def factor_loop(r_ref, tile_ref, w_ref, spread_ref, width, keep=None):
    rows, cols = r_ref.shape
    half = w_ref.shape[0]

    def store_r(i, v):
        tile_ref[i:i + 1, :] = v

    def store_w(i, v):
        w_ref[i:i + 1, :] = v

    def panel(p, carry):
        for q in range(1, rows // half):

            @pl.when(p == q)
            def _():
                a = q * half
                done = dot3(r_ref[0:a, a:a + half], r_ref[0:a, a:], 0, 0)
                r_ref[a:a + half, a:] = r_ref[a:a + half, a:] - done

        at = pl.ds(pl.multiple_of(p * half, half), half)
        factor_tile(r_ref[at, at], store_r, store_w, spread_ref, half, width)
        if keep is not None:
            keep[at, :] = w_ref[...]
        for q in range(rows // half):

            @pl.when(p == q)
            def _():
                a = q * half
                if a:
                    r_ref[a:a + half, 0:a] = jnp.zeros((half, a), f32)
                if a + half < cols:
                    r_ref[a:a + half, a + half:] = dot3(w_ref[...], r_ref[a:a + half, a + half:])
                r_ref[a:a + half, a:a + half] = tile_ref[...]

        return carry

    lax.fori_loop(0, rows // half, panel, 0)


def block_kernel(nprev, width, *refs):
    g_ref = refs[0]
    prev = refs[1:1 + nprev]
    r_ref = refs[1 + nprev]
    rows, cols = g_ref.shape
    u = g_ref[...]
    for t in range(nprev):
        off = prev[t].shape[1] - cols
        u = u - dot3(prev[t][:, off:off + rows], prev[t][:, off:], 0, 0)
    r_ref[...] = u
    factor_loop(*refs[1 + nprev:], width)


def factor_scratch(width):
    return [
        pltpu.VMEM((TILE, TILE), f32),
        pltpu.VMEM((TILE, TILE), f32),
        pltpu.VMEM((width * width // 2, 8, TILE), f32),
    ]


def chol_block(g, prev, width=16):
    n = len(prev)
    return pl.pallas_call(
        functools.partial(on_leader, functools.partial(block_kernel, n, width)),
        out_shape=jax.ShapeDtypeStruct(g.shape, f32),
        in_specs=[pl.BlockSpec(memory_space=pltpu.VMEM)] * (n + 1),
        out_specs=pl.BlockSpec(memory_space=pltpu.VMEM),
        scratch_shapes=factor_scratch(width),
        compiler_params=pltpu.CompilerParams(vmem_limit_bytes=12 << 20),
        cost_estimate=cost(6),
        name="factor_block",
    )(g, *prev)


def split3(x):
    high = x.astype(jnp.bfloat16)
    rest = x - high.astype(f32)
    mid = rest.astype(jnp.bfloat16)
    low = (rest - mid.astype(f32)).astype(jnp.bfloat16)
    return high, mid, low


def pick_exact(onehot, x, ca, cb, onehot_left):
    total = None
    for piece in split3(x):
        a, b = (onehot, piece) if onehot_left else (piece, onehot)
        part = lax.dot_general(a, b, (((ca,), (cb,)), ((), ())), preferred_element_type=f32)
        total = part if total is None else total + part
    return total


def route_kernel(capacity, rows_ref, row_ref, out_ref):
    n = rows_ref.shape[0]
    slots, width = out_ref.shape
    down = lax.broadcasted_iota(jnp.int32, (n, n), 0)
    across = lax.broadcasted_iota(jnp.int32, (n, n), 1)
    row = row_ref[...].astype(f32)
    column = jnp.sum(jnp.where(down == across, jnp.broadcast_to(row, (n, n)), 0.0), axis=1, keepdims=True)
    earlier = (column == row) & (down < across)
    position = jnp.sum(jnp.where(earlier, 1.0, 0.0), axis=0, keepdims=True)
    total = None
    for h in range(2):
        slot = (2 * row_ref[...] + h) * capacity + position.astype(jnp.int32)
        pick = lax.broadcasted_iota(jnp.int32, (slots, n), 0) == slot
        pick = pick.astype(f32).astype(jnp.bfloat16)
        part = pick_exact(pick, rows_ref[:, h * width:(h + 1) * width], 1, 0, True)
        total = part if total is None else total + part
    out_ref[...] = total


def route(row_values, front_of_row, fronts):
    n, width = row_values.shape
    capacity = 2 * n // fronts
    return pl.pallas_call(
        functools.partial(route_kernel, capacity),
        out_shape=jax.ShapeDtypeStruct((2 * fronts * capacity, width // 2), f32),
        in_specs=[pl.BlockSpec(memory_space=pltpu.VMEM)] * 2,
        out_specs=pl.BlockSpec(memory_space=pltpu.VMEM),
        cost_estimate=cost(3),
        name="route",
    )(row_values, front_of_row.reshape(1, n))


def gram_block(high_ref, low_ref, lo, block):
    left = high_ref[:, lo:lo + block], low_ref[:, lo:lo + block]
    return pair_dot(left, (high_ref[:, lo:], low_ref[:, lo:]), 0, 0)


def children_kernel(block, nparts, *refs):
    parts = refs[:nparts]
    columns_ref, damping_ref = refs[nparts:nparts + 2]
    outs = refs[nparts + 2:-3]
    stack_ref, high_ref, low_ref = refs[-3:]
    width = high_ref.shape[1]
    kids, rows, contrib = parts[0].shape
    each = rows * nparts
    for q in range(nparts):
        stack_ref[:, q * rows:(q + 1) * rows, :] = parts[q][...]
    parent = lax.broadcasted_iota(jnp.int32, (width, contrib), 0)

    def place(c, carry):
        spread = (parent == columns_ref[pl.ds(c, 1), :]).astype(f32).astype(jnp.bfloat16)
        high, low = split2(stack_ref[c])
        at = pl.ds(pl.multiple_of(c * each, each), each)
        high_ref[at, :] = dot16(high, spread, 1, 1).astype(jnp.bfloat16)
        low_ref[at, :] = dot16(low, spread, 1, 1).astype(jnp.bfloat16)
        return carry

    lax.fori_loop(0, kids, place, 0)
    weight = damping_ref[...]
    for s, out_ref in enumerate(outs):
        lo = s * block
        down = lax.broadcasted_iota(jnp.int32, out_ref.shape, 0)
        across = lax.broadcasted_iota(jnp.int32, out_ref.shape, 1)
        diag = jnp.where(down == across, weight[:, lo:] * weight[:, lo:], 0.0)
        out_ref[...] = diag + gram_block(high_ref, low_ref, lo, block)


def block_shapes(width, block):
    return [jax.ShapeDtypeStruct((block, width - lo), f32) for lo in range(0, width, block)]


def children_gram(parts, columns, damping, block):
    width = damping.shape[1]
    kids, rows, contrib = parts[0].shape
    shapes = block_shapes(width, block)
    return pl.pallas_call(
        functools.partial(on_leader, functools.partial(children_kernel, block, len(parts))),
        out_shape=shapes,
        in_specs=[pl.BlockSpec(memory_space=pltpu.VMEM)] * (len(parts) + 2),
        out_specs=[pl.BlockSpec(memory_space=pltpu.VMEM)] * len(shapes),
        scratch_shapes=[pltpu.VMEM((kids, rows * len(parts), contrib), f32)]
        + [pltpu.VMEM((kids * rows * len(parts), width), jnp.bfloat16)] * 2,
        compiler_params=pltpu.CompilerParams(vmem_limit_bytes=28 << 20),
        cost_estimate=cost(10),
        name="children_gram",
    )(*parts, columns, damping)


def split_parts(parts, high_ref, low_ref):
    rows = parts[0].shape[0]
    for q, part in enumerate(parts):
        at = slice(q * rows, (q + 1) * rows)
        high_ref[at, :], low_ref[at, :] = split2(part[...])


def lead_kernel(nlead, nparts, width, *refs):
    grams = refs[:nlead]
    parts = refs[nlead:nlead + nparts]
    lead_ref, top_ref, keep_ref, high_ref, low_ref = refs[nlead + nparts:nlead + nparts + 5]
    scratch = refs[nlead + nparts + 5:]
    block = grams[0].shape[0]
    cols = lead_ref.shape[1]
    split_parts(parts, high_ref, low_ref)
    for s in range(nlead):
        lo = s * block
        lead_ref[lo:lo + block, lo:] = grams[s][:, 0:cols - lo] + gram_block(high_ref, low_ref, lo, block)
    factor_loop(lead_ref, *scratch, width, keep_ref)
    top_ref[...] = lead_ref[0:block, :]


def lead_factor(grams, parts, width=16):
    block = grams[0].shape[0]
    rows, cols = parts[0].shape
    nlead = cols // block
    ins = [*grams[:nlead], *parts]
    return pl.pallas_call(
        functools.partial(on_leader, functools.partial(lead_kernel, nlead, len(parts), width)),
        out_shape=[
            jax.ShapeDtypeStruct((cols, cols), f32),
            jax.ShapeDtypeStruct((block, cols), f32),
            jax.ShapeDtypeStruct((cols, TILE), f32),
            jax.ShapeDtypeStruct((rows * len(parts), cols), jnp.bfloat16),
            jax.ShapeDtypeStruct((rows * len(parts), cols), jnp.bfloat16),
        ],
        in_specs=[pl.BlockSpec(memory_space=pltpu.VMEM)] * len(ins),
        out_specs=[pl.BlockSpec(memory_space=pltpu.VMEM)] * 5,
        scratch_shapes=factor_scratch(width),
        compiler_params=pltpu.CompilerParams(vmem_limit_bytes=20 << 20),
        cost_estimate=cost(14),
        name="lead_factor",
    )(*ins)


def cross_kernel(nblocks, nlead, nparts, *refs):
    grams = refs[:nblocks]
    parts = refs[nblocks:nblocks + nparts]
    lead_ref, keep_ref, high1_ref, low1_ref = refs[nblocks + nparts:nblocks + nparts + 4]
    outs = refs[nblocks + nparts + 4:-3]
    x_ref, high_ref, low_ref = refs[-3:]
    block = grams[0].shape[0]
    cols = lead_ref.shape[1]
    split_parts(parts, high_ref, low_ref)
    right = high_ref[...], low_ref[...]
    for s in range(nlead):
        at = slice(s * block, (s + 1) * block)
        left = high1_ref[:, at], low1_ref[:, at]
        x_ref[at, :] = grams[s][:, cols - s * block:] + pair_dot(left, right, 0, 0)
    for a in range(0, cols, TILE):
        at = slice(a, a + TILE)
        u = x_ref[at, :]
        if a:
            u = u - dot3(lead_ref[0:a, at], x_ref[0:a, :], 0, 0)
        x_ref[at, :] = dot3(keep_ref[at, :], u)
    for s in range(nlead):
        at = slice(s * block, (s + 1) * block)
        if s:
            outs[s][:, 0:cols - s * block] = lead_ref[at, s * block:]
            outs[s][:, cols - s * block:] = x_ref[at, :]
        else:
            outs[s][...] = x_ref[at, :]
    high1, low1 = split2(x_ref[...])
    for s in range(nlead, nblocks):
        lo = (s - nlead) * block
        left = high1[:, lo:lo + block], low1[:, lo:lo + block]
        done = pair_dot(left, (high1[:, lo:], low1[:, lo:]), 0, 0)
        total = grams[s][...] + gram_block(high_ref, low_ref, lo, block) - done
        if s < nblocks - 1:
            outs[s][...] = total
            continue
        for q, out_ref in enumerate(outs[s:]):
            out_ref[...] = total[q * TILE:(q + 1) * TILE, q * TILE:]


def cross_update(grams, parts, lead, keep, high1, low1):
    block = grams[0].shape[0]
    rows, cols = parts[0].shape
    nlead = cols // block
    ins = [*grams, *parts, lead, keep, high1, low1]
    shapes = [jax.ShapeDtypeStruct(g.shape, f32) for g in grams]
    shapes[0] = jax.ShapeDtypeStruct((block, grams[0].shape[1] - cols), f32)
    shapes[-1:] = [jax.ShapeDtypeStruct((TILE, block - at), f32) for at in range(0, block, TILE)]
    tall = (rows * len(parts), cols)
    return pl.pallas_call(
        functools.partial(on_leader, functools.partial(cross_kernel, len(grams), nlead, len(parts))),
        out_shape=shapes,
        in_specs=[pl.BlockSpec(memory_space=pltpu.VMEM)] * len(ins),
        out_specs=[pl.BlockSpec(memory_space=pltpu.VMEM)] * len(shapes),
        scratch_shapes=[pltpu.VMEM((cols, cols), f32)] + [pltpu.VMEM(tall, jnp.bfloat16)] * 2,
        compiler_params=pltpu.CompilerParams(vmem_limit_bytes=28 << 20),
        cost_estimate=cost(9),
        name="cross_update",
    )(*ins)


def to_leader(x, fronts, subs):
    parts = [x]
    for j in range(subs - 1):
        pairs = []
        for f in range(fronts):
            leader = leader_of(f, subs)
            near = sorted((s for s in range(subs) if s != leader), key=lambda s: (abs(s - leader), s))
            pairs.append((f * subs + near[j], f * subs + leader))
        parts.append(lax.ppermute(x, AXES, pairs))
    return parts


def from_leader(x, owner, fronts, subs):
    pairs = [(f * subs + leader_of(f, subs), f * subs + owner) for f in range(fronts)]
    return lax.ppermute(x, AXES, pairs)


def local(row_values, front_of_row, child_factors, child_columns, damping):
    fronts, subs = lax.axis_size("front"), lax.axis_size("sub")
    width = row_values.shape[1]
    block = width // subs
    kid_parts = to_leader(child_factors, fronts, subs)
    routed = route(row_values, front_of_row, fronts)
    received = lax.all_to_all(routed, "front", split_axis=0, concat_axis=0, tiled=True)
    received = received.reshape(fronts, 2, -1, width // 2)
    halves = []
    for h in range(2):
        own = received[:, h].reshape(-1, width // 2)
        halves.append(to_leader(own, fronts, subs))
    grams = children_gram(kid_parts, child_columns, damping, block)
    lead, top, keep, high1, low1 = lead_factor(grams, halves[0])
    pieces = []

    def send(x, owner, row, at):
        sent = from_leader(x, owner, fronts, subs)
        below = block - row - x.shape[0]
        pieces.append(jnp.pad(sent, ((row, below), (at, width - at - x.shape[1]))))

    nlead = subs // 2
    send(top, 0, 0, 0)
    rest = cross_update(grams, halves[1], lead, keep, high1, low1)
    send(rest[0], 0, 0, nlead * block)
    for s in range(1, nlead):
        send(rest[s], s, 0, s * block)
    factors = []
    for n, gram in enumerate(rest[nlead:]):
        owner = min(nlead + n, subs - 1)
        at = width - gram.shape[1]
        factors.append(chol_block(gram, factors))
        send(factors[-1], owner, at - owner * block, at)
    return functools.reduce(jnp.add, pieces)[None]


def solution(mesh):
    in_specs = (
        P(("front", "sub"), None),
        P(("front", "sub"), None),
        P("front", "sub", None),
        P("front", None),
        P("front", None),
    )
    out_specs = P("front", "sub", None)

    return jax.shard_map(local, mesh=mesh, in_specs=in_specs, out_specs=out_specs, check_vma=False)
```

```python
import functools

import jax
import jax.numpy as jnp
from jax import lax
from jax.experimental import pallas as pl
from jax.experimental.pallas import tpu as pltpu
from jax.sharding import PartitionSpec as P


TILE = 128
AXES = ("front", "sub")


def cost(us):
    return pl.CostEstimate(flops=int(us * 5e8), bytes_accessed=0, transcendentals=0)


f32 = jnp.float32


def leader_of(front, subs):
    return (subs // 2 - 1 + front % 2) % subs


def on_leader(body, *refs):
    @pl.when(lax.axis_index("sub") == leader_of(lax.axis_index("front"), lax.axis_size("sub")))
    def _():
        body(*refs)


def dot16(a, b, ca, cb):
    return lax.dot_general(a, b, (((ca,), (cb,)), ((), ())), preferred_element_type=f32)


def split2(x):
    high = x.astype(jnp.bfloat16)
    return high, (x - high.astype(f32)).astype(jnp.bfloat16)


def pair_dot(a, b, ca, cb):
    small = dot16(a[0], b[1], ca, cb) + dot16(a[1], b[0], ca, cb)
    return small + dot16(a[0], b[0], ca, cb)


def dot3(a, b, ca=1, cb=0):
    return pair_dot(split2(a), split2(b), ca, cb)


def rowb(v, j):
    return jnp.broadcast_to(v[j:j + 1, :], v.shape)


def factor_tile(x, store_r, store_w, spread_ref, n=128, width=16):
    lane = lax.broadcasted_iota(jnp.int32, (8, n), 1)
    sub = lax.broadcasted_iota(jnp.int32, (8, n), 0)
    lane1 = lax.broadcasted_iota(jnp.int32, (1, n), 1)
    per = width // 8
    blocks = n // width

    def spread(v, c, slot):
        spread_ref[slot] = jnp.broadcast_to(v[:, c:c + 1], v.shape)
        return spread_ref[slot]

    own = [x[8 * v:8 * v + 8, :] for v in range(per)]
    nxt = [x[width + 8 * v:width + 8 * v + 8, :] for v in range(per)]
    rest = x[2 * width:, :]
    for blk in range(blocks):
        lo = blk * width
        base = (blk % 2) * 2 * per * width
        t = list(own)
        w = [jnp.where(lane < lo, own[v], jnp.where(lane == sub + (lo + 8 * v), 1.0, 0.0)) for v in range(per)]
        b = [[None] * width for _ in range(per)]
        for c in range(width):
            for v in range(per):
                b[v][c] = spread(own[v], lo + c, base + v * width + c)
        last = blk == blocks - 1
        if not last:
            later = [[None] * width for _ in range(per)]
            for c in range(width):
                for v in range(per):
                    later[v][c] = spread(nxt[v], lo + c, base + (per + v) * width + c)
        for j in range(width):
            pv, jj = divmod(j, 8)
            here = sub == jj
            d = rowb(b[pv][j], jj)
            inv = 1.0 / d
            root = lax.rsqrt(d)
            cols = [b[v][j] for v in range(per)]
            cols[pv] = jnp.where(here, -1.0, cols[pv])
            for c in range(j + 1, width):
                row = rowb(b[pv][c], jj)
                if c == j + 1:
                    for v in range(per):
                        kept = jnp.where(here, 0.0, b[v][c]) if v == pv else b[v][c]
                        b[v][c] = kept - (cols[v] * row) * inv
                else:
                    row = row * inv
                    for v in range(per):
                        kept = jnp.where(here, 0.0, b[v][c]) if v == pv else b[v][c]
                        b[v][c] = kept - cols[v] * row
            trow, wrow = rowb(t[pv], jj), rowb(w[pv], jj)
            store_r(lo + j, jnp.where(lane1 >= lo + j, (trow * root)[0:1], 0.0))
            store_w(lo + j, (wrow * root)[0:1])
            tp, wp = trow * inv, wrow * inv
            for v in range(per):
                if last and v < pv:
                    continue
                for a, p in ((t, tp), (w, wp)):
                    kept = jnp.where(here, 0.0, a[v]) if v == pv else a[v]
                    a[v] = kept - cols[v] * p
        if last:
            break
        inside = (lane >= lo) & (lane < lo + width)
        z = [jnp.where(lane < lo + width, w[v], t[v]) for v in range(per)]
        new = []
        for v in range(per):
            terms = [later[v][c] * rowb(z[c // 8], c % 8) for c in range(width)]
            while len(terms) > 1:
                terms = [terms[q] + terms[q + 1] for q in range(0, len(terms), 2)]
            new.append(jnp.where(inside, 0.0, nxt[v]) - terms[0])
        own = new
        if rest.shape[0]:
            parts = [jnp.zeros((lo, n), f32)] if lo else []
            parts += z + [jnp.zeros((n - lo - width, n), f32)]
            zpad = jnp.concatenate(parts, axis=0)
            lane_r = lax.broadcasted_iota(jnp.int32, rest.shape, 1)
            rest = jnp.where((lane_r >= lo) & (lane_r < lo + width), 0.0, rest) - dot3(rest, zpad)
            nxt = [rest[8 * v:8 * v + 8, :] for v in range(per)]
            rest = rest[width:, :]


def factor_loop(r_ref, tile_ref, w_ref, spread_ref, width, keep=None):
    rows, cols = r_ref.shape
    half = w_ref.shape[0]

    def store_r(i, v):
        tile_ref[i:i + 1, :] = v

    def store_w(i, v):
        w_ref[i:i + 1, :] = v

    def panel(p, carry):
        for q in range(1, rows // half):

            @pl.when(p == q)
            def _():
                a = q * half
                done = dot3(r_ref[0:a, a:a + half], r_ref[0:a, a:], 0, 0)
                r_ref[a:a + half, a:] = r_ref[a:a + half, a:] - done

        at = pl.ds(pl.multiple_of(p * half, half), half)
        factor_tile(r_ref[at, at], store_r, store_w, spread_ref, half, width)
        if keep is not None:
            keep[at, :] = w_ref[...]
        for q in range(rows // half):

            @pl.when(p == q)
            def _():
                a = q * half
                if a:
                    r_ref[a:a + half, 0:a] = jnp.zeros((half, a), f32)
                if a + half < cols:
                    r_ref[a:a + half, a + half:] = dot3(w_ref[...], r_ref[a:a + half, a + half:])
                r_ref[a:a + half, a:a + half] = tile_ref[...]

        return carry

    lax.fori_loop(0, rows // half, panel, 0)


def block_kernel(nprev, width, *refs):
    g_ref = refs[0]
    prev = refs[1:1 + nprev]
    r_ref = refs[1 + nprev]
    rows, cols = g_ref.shape
    u = g_ref[...]
    for t in range(nprev):
        off = prev[t].shape[1] - cols
        u = u - dot3(prev[t][:, off:off + rows], prev[t][:, off:], 0, 0)
    r_ref[...] = u
    factor_loop(*refs[1 + nprev:], width)


def factor_scratch(width):
    return [
        pltpu.VMEM((TILE, TILE), f32),
        pltpu.VMEM((TILE, TILE), f32),
        pltpu.VMEM((width * width // 2, 8, TILE), f32),
    ]


def chol_block(g, prev, width=16):
    n = len(prev)
    return pl.pallas_call(
        functools.partial(on_leader, functools.partial(block_kernel, n, width)),
        out_shape=jax.ShapeDtypeStruct(g.shape, f32),
        in_specs=[pl.BlockSpec(memory_space=pltpu.VMEM)] * (n + 1),
        out_specs=pl.BlockSpec(memory_space=pltpu.VMEM),
        scratch_shapes=factor_scratch(width),
        compiler_params=pltpu.CompilerParams(vmem_limit_bytes=12 << 20),
        cost_estimate=cost(6),
        name="factor_block",
    )(g, *prev)


def split3(x):
    high = x.astype(jnp.bfloat16)
    rest = x - high.astype(f32)
    mid = rest.astype(jnp.bfloat16)
    low = (rest - mid.astype(f32)).astype(jnp.bfloat16)
    return high, mid, low


def pick_exact(onehot, x, ca, cb, onehot_left):
    total = None
    for piece in split3(x):
        a, b = (onehot, piece) if onehot_left else (piece, onehot)
        part = lax.dot_general(a, b, (((ca,), (cb,)), ((), ())), preferred_element_type=f32)
        total = part if total is None else total + part
    return total


def route_kernel(capacity, rows_ref, row_ref, out_ref):
    n = rows_ref.shape[0]
    slots, width = out_ref.shape
    down = lax.broadcasted_iota(jnp.int32, (n, n), 0)
    across = lax.broadcasted_iota(jnp.int32, (n, n), 1)
    row = row_ref[...].astype(f32)
    column = jnp.sum(jnp.where(down == across, jnp.broadcast_to(row, (n, n)), 0.0), axis=1, keepdims=True)
    earlier = (column == row) & (down < across)
    position = jnp.sum(jnp.where(earlier, 1.0, 0.0), axis=0, keepdims=True)
    position = position.astype(jnp.int32)
    if capacity % 8 == 0:
        half = slots // 2
        pick = lax.broadcasted_iota(jnp.int32, (half, n), 0) == row_ref[...] * capacity + position
        pick = pick.astype(f32).astype(jnp.bfloat16)
        for h in range(2):
            part = pick_exact(pick, rows_ref[:, h * width:(h + 1) * width], 1, 0, True)
            for at in range(0, half, capacity):
                to = 2 * at + h * capacity
                out_ref[to:to + capacity, :] = part[at:at + capacity, :]
        return
    total = None
    for h in range(2):
        slot = (2 * row_ref[...] + h) * capacity + position
        pick = lax.broadcasted_iota(jnp.int32, (slots, n), 0) == slot
        pick = pick.astype(f32).astype(jnp.bfloat16)
        part = pick_exact(pick, rows_ref[:, h * width:(h + 1) * width], 1, 0, True)
        total = part if total is None else total + part
    out_ref[...] = total


def route(row_values, front_of_row, fronts):
    n, width = row_values.shape
    capacity = 2 * n // fronts
    return pl.pallas_call(
        functools.partial(route_kernel, capacity),
        out_shape=jax.ShapeDtypeStruct((2 * fronts * capacity, width // 2), f32),
        in_specs=[pl.BlockSpec(memory_space=pltpu.VMEM)] * 2,
        out_specs=pl.BlockSpec(memory_space=pltpu.VMEM),
        cost_estimate=cost(3),
        name="route",
    )(row_values, front_of_row.reshape(1, n))


def gram_block(high_ref, low_ref, lo, block):
    left = high_ref[:, lo:lo + block], low_ref[:, lo:lo + block]
    return pair_dot(left, (high_ref[:, lo:], low_ref[:, lo:]), 0, 0)


def children_kernel(block, nparts, *refs):
    parts = refs[:nparts]
    columns_ref, damping_ref = refs[nparts:nparts + 2]
    outs = refs[nparts + 2:-3]
    stack_ref, high_ref, low_ref = refs[-3:]
    width = high_ref.shape[1]
    kids, rows, contrib = parts[0].shape
    each = rows * nparts
    for q in range(nparts):
        stack_ref[:, q * rows:(q + 1) * rows, :] = parts[q][...]
    parent = lax.broadcasted_iota(jnp.int32, (width, contrib), 0)

    def place(c, carry):
        spread = (parent == columns_ref[pl.ds(c, 1), :]).astype(f32).astype(jnp.bfloat16)
        high, low = split2(stack_ref[c])
        at = pl.ds(pl.multiple_of(c * each, each), each)
        high_ref[at, :] = dot16(high, spread, 1, 1).astype(jnp.bfloat16)
        low_ref[at, :] = dot16(low, spread, 1, 1).astype(jnp.bfloat16)
        return carry

    lax.fori_loop(0, kids, place, 0)
    weight = damping_ref[...]
    for s, out_ref in enumerate(outs):
        lo = s * block
        down = lax.broadcasted_iota(jnp.int32, out_ref.shape, 0)
        across = lax.broadcasted_iota(jnp.int32, out_ref.shape, 1)
        diag = jnp.where(down == across, weight[:, lo:] * weight[:, lo:], 0.0)
        out_ref[...] = diag + gram_block(high_ref, low_ref, lo, block)


def block_shapes(width, block):
    return [jax.ShapeDtypeStruct((block, width - lo), f32) for lo in range(0, width, block)]


def children_gram(parts, columns, damping, block):
    width = damping.shape[1]
    kids, rows, contrib = parts[0].shape
    shapes = block_shapes(width, block)
    return pl.pallas_call(
        functools.partial(on_leader, functools.partial(children_kernel, block, len(parts))),
        out_shape=shapes,
        in_specs=[pl.BlockSpec(memory_space=pltpu.VMEM)] * (len(parts) + 2),
        out_specs=[pl.BlockSpec(memory_space=pltpu.VMEM)] * len(shapes),
        scratch_shapes=[pltpu.VMEM((kids, rows * len(parts), contrib), f32)]
        + [pltpu.VMEM((kids * rows * len(parts), width), jnp.bfloat16)] * 2,
        compiler_params=pltpu.CompilerParams(vmem_limit_bytes=28 << 20),
        cost_estimate=cost(10),
        name="children_gram",
    )(*parts, columns, damping)


def split_parts(parts, high_ref, low_ref):
    rows = parts[0].shape[0]
    for q, part in enumerate(parts):
        at = slice(q * rows, (q + 1) * rows)
        high_ref[at, :], low_ref[at, :] = split2(part[...])


def lead_kernel(nlead, nparts, width, *refs):
    grams = refs[:nlead]
    parts = refs[nlead:nlead + nparts]
    lead_ref, top_ref, keep_ref, high_ref, low_ref = refs[nlead + nparts:nlead + nparts + 5]
    scratch = refs[nlead + nparts + 5:]
    block = grams[0].shape[0]
    cols = lead_ref.shape[1]
    split_parts(parts, high_ref, low_ref)
    for s in range(nlead):
        lo = s * block
        lead_ref[lo:lo + block, lo:] = grams[s][:, 0:cols - lo] + gram_block(high_ref, low_ref, lo, block)
    factor_loop(lead_ref, *scratch, width, keep_ref)
    top_ref[...] = lead_ref[0:block, :]


def lead_factor(grams, parts, width=16):
    block = grams[0].shape[0]
    rows, cols = parts[0].shape
    nlead = cols // block
    ins = [*grams[:nlead], *parts]
    return pl.pallas_call(
        functools.partial(on_leader, functools.partial(lead_kernel, nlead, len(parts), width)),
        out_shape=[
            jax.ShapeDtypeStruct((cols, cols), f32),
            jax.ShapeDtypeStruct((block, cols), f32),
            jax.ShapeDtypeStruct((cols, TILE), f32),
            jax.ShapeDtypeStruct((rows * len(parts), cols), jnp.bfloat16),
            jax.ShapeDtypeStruct((rows * len(parts), cols), jnp.bfloat16),
        ],
        in_specs=[pl.BlockSpec(memory_space=pltpu.VMEM)] * len(ins),
        out_specs=[pl.BlockSpec(memory_space=pltpu.VMEM)] * 5,
        scratch_shapes=factor_scratch(width),
        compiler_params=pltpu.CompilerParams(vmem_limit_bytes=20 << 20),
        cost_estimate=cost(14),
        name="lead_factor",
    )(*ins)


def cross_kernel(nblocks, nlead, nparts, *refs):
    grams = refs[:nblocks]
    parts = refs[nblocks:nblocks + nparts]
    lead_ref, keep_ref, high1_ref, low1_ref = refs[nblocks + nparts:nblocks + nparts + 4]
    outs = refs[nblocks + nparts + 4:-3]
    x_ref, high_ref, low_ref = refs[-3:]
    block = grams[0].shape[0]
    cols = lead_ref.shape[1]
    split_parts(parts, high_ref, low_ref)
    right = high_ref[...], low_ref[...]
    for s in range(nlead):
        at = slice(s * block, (s + 1) * block)
        left = high1_ref[:, at], low1_ref[:, at]
        x_ref[at, :] = grams[s][:, cols - s * block:] + pair_dot(left, right, 0, 0)
    for a in range(0, cols, TILE):
        at = slice(a, a + TILE)
        u = x_ref[at, :]
        if a:
            u = u - dot3(lead_ref[0:a, at], x_ref[0:a, :], 0, 0)
        x_ref[at, :] = dot3(keep_ref[at, :], u)
    for s in range(nlead):
        at = slice(s * block, (s + 1) * block)
        if s:
            outs[s][:, 0:cols - s * block] = lead_ref[at, s * block:]
            outs[s][:, cols - s * block:] = x_ref[at, :]
        else:
            outs[s][...] = x_ref[at, :]
    high1, low1 = split2(x_ref[...])
    for s in range(nlead, nblocks):
        lo = (s - nlead) * block
        left = high1[:, lo:lo + block], low1[:, lo:lo + block]
        done = pair_dot(left, (high1[:, lo:], low1[:, lo:]), 0, 0)
        total = grams[s][...] + gram_block(high_ref, low_ref, lo, block) - done
        if s < nblocks - 1:
            outs[s][...] = total
            continue
        for q, out_ref in enumerate(outs[s:]):
            out_ref[...] = total[q * TILE:(q + 1) * TILE, q * TILE:]


def cross_update(grams, parts, lead, keep, high1, low1):
    block = grams[0].shape[0]
    rows, cols = parts[0].shape
    nlead = cols // block
    ins = [*grams, *parts, lead, keep, high1, low1]
    shapes = [jax.ShapeDtypeStruct(g.shape, f32) for g in grams]
    shapes[0] = jax.ShapeDtypeStruct((block, grams[0].shape[1] - cols), f32)
    shapes[-1:] = [jax.ShapeDtypeStruct((TILE, block - at), f32) for at in range(0, block, TILE)]
    tall = (rows * len(parts), cols)
    return pl.pallas_call(
        functools.partial(on_leader, functools.partial(cross_kernel, len(grams), nlead, len(parts))),
        out_shape=shapes,
        in_specs=[pl.BlockSpec(memory_space=pltpu.VMEM)] * len(ins),
        out_specs=[pl.BlockSpec(memory_space=pltpu.VMEM)] * len(shapes),
        scratch_shapes=[pltpu.VMEM((cols, cols), f32)] + [pltpu.VMEM(tall, jnp.bfloat16)] * 2,
        compiler_params=pltpu.CompilerParams(vmem_limit_bytes=28 << 20),
        cost_estimate=cost(9),
        name="cross_update",
    )(*ins)


def to_leader(x, fronts, subs):
    parts = [x]
    for j in range(subs - 1):
        pairs = []
        for f in range(fronts):
            leader = leader_of(f, subs)
            near = sorted((s for s in range(subs) if s != leader), key=lambda s: (abs(s - leader), s))
            pairs.append((f * subs + near[j], f * subs + leader))
        parts.append(lax.ppermute(x, AXES, pairs))
    return parts


def from_leader(x, owner, fronts, subs):
    pairs = [(f * subs + leader_of(f, subs), f * subs + owner) for f in range(fronts)]
    return lax.ppermute(x, AXES, pairs)


def local(row_values, front_of_row, child_factors, child_columns, damping):
    fronts, subs = lax.axis_size("front"), lax.axis_size("sub")
    width = row_values.shape[1]
    block = width // subs
    kid_parts = to_leader(child_factors, fronts, subs)
    routed = route(row_values, front_of_row, fronts)
    received = lax.all_to_all(routed, "front", split_axis=0, concat_axis=0, tiled=True)
    received = received.reshape(fronts, 2, -1, width // 2)
    halves = []
    for h in range(2):
        own = received[:, h].reshape(-1, width // 2)
        halves.append(to_leader(own, fronts, subs))
    grams = children_gram(kid_parts, child_columns, damping, block)
    lead, top, keep, high1, low1 = lead_factor(grams, halves[0])
    pieces = []

    def send(x, owner, row, at):
        sent = from_leader(x, owner, fronts, subs)
        below = block - row - x.shape[0]
        pieces.append(jnp.pad(sent, ((row, below), (at, width - at - x.shape[1]))))

    nlead = subs // 2
    send(top, 0, 0, 0)
    rest = cross_update(grams, halves[1], lead, keep, high1, low1)
    send(rest[0], 0, 0, nlead * block)
    for s in range(1, nlead):
        send(rest[s], s, 0, s * block)
    factors = []
    for n, gram in enumerate(rest[nlead:]):
        owner = min(nlead + n, subs - 1)
        at = width - gram.shape[1]
        factors.append(chol_block(gram, factors))
        send(factors[-1], owner, at - owner * block, at)
    return functools.reduce(jnp.add, pieces)[None]


def solution(mesh):
    in_specs = (
        P(("front", "sub"), None),
        P(("front", "sub"), None),
        P("front", "sub", None),
        P("front", None),
        P("front", None),
    )
    out_specs = P("front", "sub", None)

    return jax.shard_map(local, mesh=mesh, in_specs=in_specs, out_specs=out_specs, check_vma=False)
```
